16 devices in a mesh: dp: 4 (over z, y), tp: 4 (over x, core).
Axes of the slice: x: 2, y: 2, z: 2, core: 2. Of those that a mesh axis runs over, the one named last changes fastest.
Arguments:
- hidden: bfloat16 [128, 3072], P('dp'), parts along dimension 0
- final_gain: bfloat16 [3072], replicated
- embed_table: bfloat16 [128256, 3072], P(None, 'tp')
- targets: int32 [128], P('dp'), parts along dimension 0
- temperature: float32 [], replicated
Outputs:
- output 1: float32 [128], P('dp'), parts along dimension 0
- output 2: float32 [128], P('dp'), parts along dimension 0
- output 3: bfloat16 [128, 128256], P('dp', 'tp'), parts along dimension 0
There are 4 independent parts. The reference program is written for one: setup_inputs(seed, part) draws one part's arguments, and reference() takes and returns one part's arrays. A program takes and returns all parts, laid end to end along the dimension named above; an argument that names none is the same for every part.
All inputs are finite; a program needn't handle non-finite values.
Results may differ from the reference program's by a relative error of at most 0.001.
Values sent between devices are 32-bit elements.
A program may use at most 1 GiB of HBM per device.

```python
import jax
import jax.numpy as jnp
from jax import lax

TOKENS = 32
HIDDEN = 3072
VOCABULARY = 128256
NORM_EPS = 1e-6
ROW_BLOCK = min(TOKENS, 32)


def setup_inputs(seed: int = 0, part: int = 0) -> dict:
    shared_key, part_root = jax.random.split(jax.random.key(seed))
    part_key = jax.random.fold_in(part_root, part)
    gain_key, table_key, temp_key = jax.random.split(shared_key, 3)
    hidden_key, perm_key, offset_key = jax.random.split(part_key, 3)
    hidden = jax.random.normal(hidden_key, (TOKENS, HIDDEN), jnp.float32).astype(jnp.bfloat16)
    final_gain = jax.random.uniform(gain_key, (HIDDEN,), jnp.float32, 0.5, 1.5).astype(jnp.bfloat16)
    embed_table = (jax.random.normal(table_key, (VOCABULARY, HIDDEN), jnp.float32) * (2.0 / HIDDEN ** 0.5)).astype(jnp.bfloat16)
    stride = VOCABULARY // TOKENS
    targets = (jax.random.permutation(perm_key, TOKENS).astype(jnp.int32) * stride
               + jax.random.randint(offset_key, (TOKENS,), 0, stride, jnp.int32))
    temperature = jax.random.uniform(temp_key, (), jnp.float32, 0.8, 1.25)
    return {'hidden': hidden, 'final_gain': final_gain, 'embed_table': embed_table,
            'targets': targets, 'temperature': temperature}


def reference(hidden, final_gain, embed_table, targets, temperature):
    hidden_f32 = hidden.astype(jnp.float32)
    inv_rms = lax.rsqrt(jnp.mean(hidden_f32 * hidden_f32, axis=-1, keepdims=True) + NORM_EPS)
    normed = (hidden_f32 * inv_rms * final_gain.astype(jnp.float32)).astype(jnp.bfloat16)
    num_blocks = TOKENS // ROW_BLOCK
    normed_blocks = normed.reshape(num_blocks, ROW_BLOCK, HIDDEN)
    target_blocks = targets.reshape(num_blocks, ROW_BLOCK)

    def score_block(block_pair):
        normed_rows, target_ids = block_pair
        logits = jnp.dot(normed_rows, embed_table.T, preferred_element_type=jnp.float32) / temperature
        row_max = jnp.max(logits, axis=-1, keepdims=True)
        log_norm = row_max[:, 0] + jnp.log(jnp.sum(jnp.exp(logits - row_max), axis=-1))
        target_logit = jnp.take_along_axis(logits, target_ids[:, None], axis=1)[:, 0]
        token_probs = jnp.exp(logits - log_norm[:, None]).astype(jnp.bfloat16)
        return log_norm, target_logit - log_norm, token_probs

    log_norm, target_logprob, token_probs = lax.map(score_block, (normed_blocks, target_blocks))
    return (log_norm.reshape(TOKENS), target_logprob.reshape(TOKENS),
            token_probs.reshape(TOKENS, VOCABULARY))
```

```python
import functools

import jax
import jax.numpy as jnp
from jax import lax
from jax.experimental import pallas as pl
from jax.experimental.pallas import tpu as pltpu
from jax.sharding import PartitionSpec as P

NORM_EPS = 1e-6
MESH = pl.DeviceIdType.MESH
F32 = jnp.float32
BF16 = jnp.bfloat16
G = 4
R = 256
NBUF = 8


def scores_kernel(dims, temp_ref, tgt_ref, hid_hbm, gain_hbm, table, logits_ref, stats_ref, lncol_ref,
                  hid, gain, w, ring, tail, ps, po, ls, lo, ra, rb, rx, acc, st,
                  in_sem, ring_sem, tail_sem, as_sem, ar_sem, bs_sem, br_sem, xs_sem, xr_sem, ss_sem, sr_sem):
    tokens, hidden_size, width, vq, nf, rt = dims
    me = lax.axis_index('tp')
    x = me // 2
    c = me % 2
    sib = 2 * x + (1 - c)
    xpeer = 2 * (1 - x) + c
    diag = 2 * (1 - x) + (1 - c)
    rows = G * R
    trows = G * rt
    last = nf * R
    steps = 4 * nf

    def table_copy(s):
        phase = s // (2 * nf)
        j = s - phase * (2 * nf)
        k = j // 2
        which = j - 2 * k
        xx = (1 - phase) * (1 - x) + phase * x
        cc = (1 - which) * (1 - c) + which * c
        start = pl.multiple_of((2 * xx + cc) * vq + k * rows, 64)
        slot = s % NBUF
        return pltpu.make_async_copy(table.at[pl.ds(start, rows)], ring.at[slot], ring_sem.at[slot])

    def tail_copy(i):
        xx = (1 - x) if i < 2 else x
        cc = (1 - c) if i % 2 == 0 else c
        start = pl.multiple_of((2 * xx + cc) * vq + nf * rows, 64)
        return pltpu.make_async_copy(table.at[pl.ds(start, trows)], tail.at[i], tail_sem.at[i])

    def chunk(k):
        return pl.ds(pl.multiple_of(k * R, R), R)

    tail_rows = pl.ds(last, rt)

    def remote(src, dst, send, recv, k, sl, dev):
        return pltpu.make_async_remote_copy(src_ref=src.at[sl], dst_ref=dst.at[sl], send_sem=send.at[k],
                                            recv_sem=recv.at[k], device_id={'tp': dev}, device_id_type=MESH)

    def a_copy(k, sl):
        return remote(ps, ra, as_sem, ar_sem, k, sl, sib)

    def b_copy(k, sl):
        return remote(ls, rb, bs_sem, br_sem, k, sl, sib)

    def x_copy(k, sl):
        return remote(po, rx, xs_sem, xr_sem, k, sl, xpeer)

    hid_copy = pltpu.make_async_copy(hid_hbm, hid, in_sem.at[0])
    gain_copy = pltpu.make_async_copy(gain_hbm, gain, in_sem.at[1])
    hid_copy.start()
    gain_copy.start()
    for s in range(NBUF):
        table_copy(s).start()
    for i in range(4):
        tail_copy(i).start()

    barrier = pltpu.get_barrier_semaphore()
    for peer in (sib, xpeer, diag):
        pl.semaphore_signal(barrier, inc=1, device_id={'tp': peer}, device_id_type=MESH)

    hid_copy.wait()
    gain_copy.wait()
    hf = hid[...].astype(F32)
    inv = lax.rsqrt(jnp.mean(hf * hf, axis=-1, keepdims=True) + NORM_EPS)
    cols = pl.ds(pl.multiple_of(me * width, 128), width)
    u = (hid[:, cols].astype(F32) * inv * gain[:, cols].astype(F32)).astype(BF16).astype(F32)
    u_t = jnp.concatenate([u] * G, axis=0).T
    group = lax.broadcasted_iota(jnp.int32, (width, 128), 1) // tokens
    for g in range(G):
        w[g * width:(g + 1) * width, :] = jnp.where(group == g, u_t, 0.0).astype(BF16)
    acc[0] = jnp.full((8, 128), -jnp.inf, F32)
    acc[1] = jnp.zeros((8, 128), F32)
    acc[2] = jnp.zeros((8, 128), F32)
    pl.semaphore_wait(barrier, 3)

    def packed_dot(view, n):
        total = None
        for g in range(G):
            part = jnp.dot(view[g * n:(g + 1) * n, :], w[g * width:(g + 1) * width, :], preferred_element_type=F32)
            total = part if total is None else total + part
        return total

    def ring_dot(s, dst, sl):
        table_copy(s).wait()
        dst[sl, :] = packed_dot(ring.at[s % NBUF], R)

        @pl.when(s + NBUF < steps)
        def _():
            table_copy(s + NBUF).start()

    def add_sibling(k, sl):
        a_copy(k, sl).wait_recv()
        po[sl, :] = po[sl, :] + ra[sl, :]

    @pl.loop(0, nf)
    def _(k):
        ring_dot(2 * k, ps, chunk(k))

        @pl.when(k > 0)
        def _():
            add_sibling(k - 1, chunk(k - 1))

        a_copy(k, chunk(k)).start()
        ring_dot(2 * k + 1, po, chunk(k))

        @pl.when(k > 0)
        def _():
            x_copy(k - 1, chunk(k - 1)).start()

    tail_copy(0).wait()
    ps[tail_rows, :] = packed_dot(tail.at[0], rt)
    add_sibling(nf - 1, chunk(nf - 1))
    a_copy(nf, tail_rows).start()
    tail_copy(1).wait()
    po[tail_rows, :] = packed_dot(tail.at[1], rt)
    x_copy(nf - 1, chunk(nf - 1)).start()

    @pl.loop(0, nf)
    def _(k):
        ring_dot(2 * nf + 2 * k, ls, chunk(k))

        @pl.when(k == 0)
        def _():
            add_sibling(nf, tail_rows)

        ring_dot(2 * nf + 2 * k + 1, lo, chunk(k))

        @pl.when(k == 0)
        def _():
            x_copy(nf, tail_rows).start()

        b_copy(k, chunk(k)).start()

    tail_copy(2).wait()
    ls[tail_rows, :] = packed_dot(tail.at[2], rt)
    tail_copy(3).wait()
    lo[tail_rows, :] = packed_dot(tail.at[3], rt)
    b_copy(nf, tail_rows).start()

    temp = temp_ref[0, 0]
    lane_group = lax.broadcasted_iota(jnp.int32, (1, 128), 1) // tokens
    tgt = tgt_ref[...] - me * vq

    def logits_of(k, sl):
        b_copy(k, sl).wait_recv()
        x_copy(k, sl).wait_recv()
        return (lo[sl, :] + rb[sl, :] + rx[sl, :]) / temp

    def update(t, n, base):
        t3 = t.reshape(n // 8, 8, 128)
        m_old = acc[0]
        m_new = jnp.maximum(m_old, jnp.max(t3, axis=0))
        acc[0] = m_new
        acc[1] = acc[1] * jnp.exp(m_old - m_new) + jnp.sum(jnp.exp(t3 - m_new), axis=0)
        row = lax.broadcasted_iota(jnp.int32, (n, 128), 0)
        hit = row == (tgt - base - lane_group * n)
        acc[2] += jnp.sum(jnp.where(hit, t, 0.0).reshape(n // 8, 8, 128), axis=0)

    @pl.loop(0, nf)
    def _(k):
        t = logits_of(k, chunk(k))
        update(t, R, k * rows)
        tt = t.T
        for g in range(G):
            logits_ref[:, pl.ds(pl.multiple_of(k * rows + g * R, 128), R)] = tt[g * tokens:(g + 1) * tokens, :]

    t = logits_of(nf, tail_rows)
    update(t, rt, nf * rows)

    m = jnp.max(acc[0], axis=0, keepdims=True)
    for shift in (32, 64):
        m = jnp.maximum(m, pltpu.roll(m, shift, 1))
    total = jnp.sum(acc[1] * jnp.exp(acc[0] - m), axis=0, keepdims=True)
    hit = jnp.sum(acc[2], axis=0, keepdims=True)
    for shift in (32, 64):
        total = total + pltpu.roll(total, shift, 1)
        hit = hit + pltpu.roll(hit, shift, 1)
    st[me] = jnp.concatenate([m, total, hit, jnp.zeros((5, 128), F32)], axis=0)

    tt = jnp.concatenate([t, jnp.zeros((128 - rt, 128), F32)], axis=0).T
    parts = [tt[g * tokens:(g + 1) * tokens, :] for g in range(G)]
    lane = lax.broadcasted_iota(jnp.int32, (tokens, 128), 1)
    for i in range((G * rt + 127) // 128):
        tile = jnp.zeros((tokens, 128), F32)
        for g in range(G):
            off = g * rt - i * 128
            if off <= -rt or off >= 128:
                continue
            moved = pltpu.roll(parts[g], off % 128, 1) if off % 128 else parts[g]
            tile = jnp.where((lane >= off) & (lane < off + rt), moved, tile)
        logits_ref[:, nf * rows + i * 128:nf * rows + (i + 1) * 128] = tile

    stat_copies = []
    for i, peer in enumerate((sib, xpeer, diag)):
        copy = pltpu.make_async_remote_copy(src_ref=st.at[me], dst_ref=st.at[me], send_sem=ss_sem.at[i],
                                            recv_sem=sr_sem.at[i], device_id={'tp': peer}, device_id_type=MESH)
        copy.start()
        stat_copies.append(copy)
    for copy in stat_copies:
        copy.wait_recv()
    ms = [st[i, 0:1, :] for i in range(4)]
    top = jnp.maximum(jnp.maximum(ms[0], ms[1]), jnp.maximum(ms[2], ms[3]))
    norm = jnp.zeros((1, 128), F32)
    hit = jnp.zeros((1, 128), F32)
    for i in range(4):
        norm = norm + st[i, 1:2, :] * jnp.exp(ms[i] - top)
        hit = hit + st[i, 2:3, :]
    log_norm = top + jnp.log(norm)
    stats_ref[...] = jnp.concatenate([log_norm, hit - log_norm, jnp.zeros((6, 128), F32)], axis=0)
    lncol_ref[...] = jnp.broadcast_to(log_norm, (128, 128)).T[:tokens, :]

    for copy in stat_copies:
        copy.wait_send()

    @pl.loop(0, nf)
    def _(k):
        a_copy(k, chunk(k)).wait_send()
        b_copy(k, chunk(k)).wait_send()
        x_copy(k, chunk(k)).wait_send()

    a_copy(nf, tail_rows).wait_send()
    b_copy(nf, tail_rows).wait_send()
    x_copy(nf, tail_rows).wait_send()


def probs_kernel(logits_ref, stats_ref, lncol_ref, ln_ref, tl_ref, probs_ref):
    @pl.when(pl.program_id(0) == 0)
    def _():
        ln_ref[...] = stats_ref[0:1, :32]
        tl_ref[...] = stats_ref[1:2, :32]

    probs_ref[...] = jnp.exp(logits_ref[...] - lncol_ref[:, 0:1]).astype(BF16)


def solution(mesh):
    def local_scores(hidden, final_gain, table, targets, temperature):
        tokens, hidden_size = hidden.shape
        vocab, width = table.shape
        vq = vocab // 4
        nf = vq // (G * R)
        rt = (vq - nf * G * R) // G
        packed = vq // G
        lanes = (vq + 127) // 128 * 128
        dims = (tokens, hidden_size, width, vq, nf, rt)
        tgt = jnp.tile(targets, G).reshape(1, G * tokens)
        vmem = pl.BlockSpec(memory_space=pltpu.VMEM)
        anyspace = pl.BlockSpec(memory_space=pl.ANY)
        nsem = nf + 1
        logits, stats, lncol = pl.pallas_call(
            functools.partial(scores_kernel, dims),
            out_shape=(jax.ShapeDtypeStruct((tokens, lanes), F32),
                       jax.ShapeDtypeStruct((8, 128), F32),
                       jax.ShapeDtypeStruct((tokens, 128), F32)),
            in_specs=[pl.BlockSpec(memory_space=pltpu.SMEM), vmem, anyspace, anyspace, anyspace],
            out_specs=(vmem, vmem, vmem),
            scratch_shapes=[
                pltpu.VMEM((tokens, hidden_size), BF16),
                pltpu.VMEM((1, hidden_size), BF16),
                pltpu.VMEM((G * width, 128), BF16),
                pltpu.VMEM((NBUF, G * R, width), BF16),
                pltpu.VMEM((4, G * rt, width), BF16),
            ] + [pltpu.VMEM((packed, 128), F32)] * 7 + [
                pltpu.VMEM((3, 8, 128), F32),
                pltpu.VMEM((4, 8, 128), F32),
                pltpu.SemaphoreType.DMA((2,)),
                pltpu.SemaphoreType.DMA((NBUF,)),
                pltpu.SemaphoreType.DMA((4,)),
            ] + [pltpu.SemaphoreType.DMA((nsem,))] * 6 + [
                pltpu.SemaphoreType.DMA((3,)),
                pltpu.SemaphoreType.DMA((3,)),
            ],
            compiler_params=pltpu.CompilerParams(collective_id=0, has_side_effects=True,
                                                 vmem_limit_bytes=56 * 2 ** 20),
        )(temperature.reshape(1, 1), tgt, hidden, final_gain.reshape(1, hidden_size), table)
        block = 8192
        log_norm, target_logprob, probs = pl.pallas_call(
            probs_kernel,
            grid=(pl.cdiv(vq, block),),
            out_shape=(jax.ShapeDtypeStruct((1, tokens), F32),
                       jax.ShapeDtypeStruct((1, tokens), F32),
                       jax.ShapeDtypeStruct((tokens, vq), BF16)),
            in_specs=[pl.BlockSpec((tokens, block), lambda i: (0, i)),
                      pl.BlockSpec((8, 128), lambda i: (0, 0)),
                      pl.BlockSpec((tokens, 128), lambda i: (0, 0))],
            out_specs=(pl.BlockSpec((1, tokens), lambda i: (0, 0)),
                       pl.BlockSpec((1, tokens), lambda i: (0, 0)),
                       pl.BlockSpec((tokens, block), lambda i: (0, i))),
        )(logits, stats, lncol)
        return log_norm.reshape(tokens), target_logprob.reshape(tokens), probs

    return jax.shard_map(local_scores, mesh=mesh,
                         in_specs=(P('dp', None), P(None), P(None, 'tp'), P('dp'), P()),
                         out_specs=(P('dp'), P('dp'), P('dp', 'tp')),
                         check_vma=False)
```

```python
import functools

import jax
import jax.numpy as jnp
from jax import lax
from jax.experimental import pallas as pl
from jax.experimental.pallas import tpu as pltpu
from jax.sharding import PartitionSpec as P

NORM_EPS = 1e-6
MESH = pl.DeviceIdType.MESH
F32 = jnp.float32
BF16 = jnp.bfloat16
G = 4
R = 256
NBUF = 8
PIECES = 2


def scores_kernel(dims, temp_ref, tgt_hbm, hid_hbm, gain_hbm, table, logits_ref, stats_ref, lncol_ref,
                  tgt_ref, hid, gain, gain32, w, ring, tail, ps, po, ls, lo, ra, rb, rx, st,
                  in_sem, ring_sem, tail_sem, as_sem, ar_sem, bs_sem, br_sem, xs_sem, xr_sem, ss_sem, sr_sem):
    tokens, hidden_size, width, vq, nf, rt = dims
    me = lax.axis_index('tp')
    x = me // 2
    c = me % 2
    sib = 2 * x + (1 - c)
    xpeer = 2 * (1 - x) + c
    diag = 2 * (1 - x) + (1 - c)
    rows = G * R
    trows = G * rt
    last = nf - 1
    steps = 4 * nf

    def table_copy(s):
        phase = s // (2 * nf)
        j = s - phase * (2 * nf)
        k = j // 2
        which = j - 2 * k
        xx = (1 - phase) * (1 - x) + phase * x
        cc = (1 - which) * (1 - c) + which * c
        start = pl.multiple_of((2 * xx + cc) * vq + k * rows, 64)
        slot = s % NBUF
        return pltpu.make_async_copy(table.at[pl.ds(start, rows)], ring.at[slot], ring_sem.at[slot])

    def tail_copy(i):
        xx = (1 - x) if i < 2 else x
        cc = (1 - c) if i % 2 == 0 else c
        start = pl.multiple_of((2 * xx + cc) * vq + nf * rows, 64)
        return pltpu.make_async_copy(table.at[pl.ds(start, trows)], tail.at[i], tail_sem.at[i])

    def chunk(k):
        return pl.ds(pl.multiple_of(k * R, R), R)

    tail_rows = pl.ds(nf * R, rt)

    def remote(src, dst, send, recv, k, sl, dev):
        return pltpu.make_async_remote_copy(src_ref=src.at[sl], dst_ref=dst.at[sl], send_sem=send.at[k],
                                            recv_sem=recv.at[k], device_id={'tp': dev}, device_id_type=MESH)

    def a_copy(k, sl):
        return remote(ps, ra, as_sem, ar_sem, k, sl, sib)

    def b_copy(k, sl):
        return remote(ls, rb, bs_sem, br_sem, k, sl, sib)

    def x_copy(k, sl):
        return remote(po, rx, xs_sem, xr_sem, k, sl, xpeer)

    piece = R // PIECES

    def x_piece(p):
        return x_copy(last if p == 0 else nf + p, pl.ds(last * R + p * piece, piece))

    hid_copy = pltpu.make_async_copy(hid_hbm, hid, in_sem.at[0])
    gain_copy = pltpu.make_async_copy(gain_hbm, gain, in_sem.at[1])
    tgt_copy = pltpu.make_async_copy(tgt_hbm, tgt_ref, in_sem.at[2])
    hid_copy.start()
    gain_copy.start()
    tail_copy(0).start()
    tail_copy(1).start()
    for s in range(NBUF):
        table_copy(s).start()
    tgt_copy.start()
    tail_copy(2).start()
    tail_copy(3).start()

    barrier = pltpu.get_barrier_semaphore()
    for peer in (sib, xpeer, diag):
        pl.semaphore_signal(barrier, inc=1, device_id={'tp': peer}, device_id_type=MESH)

    hid_copy.wait()
    gain_copy.wait()
    hf = hid[...].astype(F32)
    inv = lax.rsqrt(jnp.mean(hf * hf, axis=-1, keepdims=True) + NORM_EPS)
    cols = pl.ds(pl.multiple_of(me * width, 128), width)
    gain32[...] = gain[...].astype(F32)
    scaled = hid[:, cols].astype(F32) * inv
    u = jnp.concatenate([scaled[:, j * 128:(j + 1) * 128] * gain32[pl.ds(me * (width // 128) + j, 1), :]
                         for j in range(width // 128)], axis=1).astype(BF16).astype(F32)
    u_t = jnp.concatenate([u] * G, axis=0).T
    group = lax.broadcasted_iota(jnp.int32, (width, 128), 1) // tokens
    for g in range(G):
        w[g * width:(g + 1) * width, :] = jnp.where(group == g, u_t, 0.0).astype(BF16)
    pl.semaphore_wait(barrier, 3)

    def packed_dot(view, n):
        total = None
        for g in range(G):
            part = jnp.dot(view[g * n:(g + 1) * n, :], w[g * width:(g + 1) * width, :], preferred_element_type=F32)
            total = part if total is None else total + part
        return total

    def ring_dot(s, dst, sl):
        table_copy(s).wait()
        dst[sl, :] = packed_dot(ring.at[s % NBUF], R)

        @pl.when(s + NBUF < steps)
        def _():
            table_copy(s + NBUF).start()

    def add_sibling(k, sl):
        a_copy(k, sl).wait_recv()
        po[sl, :] = po[sl, :] + ra[sl, :]

    tail_copy(0).wait()
    ps[tail_rows, :] = packed_dot(tail.at[0], rt)
    a_copy(nf, tail_rows).start()
    tail_copy(1).wait()
    po[tail_rows, :] = packed_dot(tail.at[1], rt)

    @pl.loop(0, nf)
    def _(k):
        ring_dot(2 * k, ps, chunk(k))
        a_copy(k, chunk(k)).start()

        @pl.when(k == 0)
        def _():
            add_sibling(nf, tail_rows)
            x_copy(nf, tail_rows).start()

        @pl.when(k > 0)
        def _():
            add_sibling(k - 1, chunk(k - 1))

        @pl.when(k == 1)
        def _():
            x_copy(k - 1, chunk(k - 1)).start()

        ring_dot(2 * k + 1, po, chunk(k))

        @pl.when(k > 1)
        def _():
            x_copy(k - 1, chunk(k - 1)).start()

    acc = st.at[me]
    acc[0] = jnp.full((8, 128), -jnp.inf, F32)
    acc[1] = jnp.zeros((8, 128), F32)
    acc[2] = jnp.zeros((8, 128), F32)
    tail_copy(2).wait()
    ls[tail_rows, :] = packed_dot(tail.at[2], rt)
    tail_copy(3).wait()
    lo[tail_rows, :] = packed_dot(tail.at[3], rt)
    add_sibling(last, chunk(last))

    @pl.loop(0, nf)
    def _(k):
        ring_dot(2 * nf + 2 * k, ls, chunk(k))

        @pl.when(k == 0)
        def _():
            b_copy(nf, tail_rows).start()
            for p in range(PIECES):
                x_piece(p).start()

        ring_dot(2 * nf + 2 * k + 1, lo, chunk(k))
        b_copy(k, chunk(k)).start()

    tgt_copy.wait()
    temp = temp_ref[0, 0]
    lane_group = lax.broadcasted_iota(jnp.int32, (1, 128), 1) // tokens
    tgt = jnp.concatenate([tgt_ref[...]] * G, axis=1) - me * vq

    def update(sl, n, base, stride):
        t = (lo[sl, :] + rb[sl, :] + rx[sl, :]) / temp
        t3 = t.reshape(n // 8, 8, 128)
        m_old = acc[0]
        m_new = jnp.maximum(m_old, jnp.max(t3, axis=0))
        acc[0] = m_new
        acc[1] = acc[1] * jnp.exp(m_old - m_new) + jnp.sum(jnp.exp(t3 - m_new), axis=0)
        row = lax.broadcasted_iota(jnp.int32, (n, 128), 0)
        hit = row == (tgt - base - lane_group * stride)
        acc[2] += jnp.sum(jnp.where(hit, t, 0.0).reshape(n // 8, 8, 128), axis=0)
        return t

    def put(t, n, base, stride):
        tt = t.T
        for g in range(G):
            logits_ref[:, pl.ds(pl.multiple_of(base + g * stride, 128), n)] = tt[g * tokens:(g + 1) * tokens, :]

    b_copy(nf, tail_rows).wait_recv()
    x_copy(nf, tail_rows).wait_recv()
    t = update(tail_rows, rt, nf * rows, rt)
    tt = jnp.concatenate([t, jnp.zeros((128 - rt, 128), F32)], axis=0).T
    parts = [tt[g * tokens:(g + 1) * tokens, :] for g in range(G)]
    lane = lax.broadcasted_iota(jnp.int32, (tokens, 128), 1)
    for i in range((G * rt + 127) // 128):
        tile = jnp.zeros((tokens, 128), F32)
        for g in range(G):
            off = g * rt - i * 128
            if off <= -rt or off >= 128:
                continue
            moved = pltpu.roll(parts[g], off % 128, 1) if off % 128 else parts[g]
            tile = jnp.where((lane >= off) & (lane < off + rt), moved, tile)
        logits_ref[:, nf * rows + i * 128:nf * rows + (i + 1) * 128] = tile

    @pl.loop(0, last)
    def _(k):
        b_copy(k, chunk(k)).wait_recv()
        x_copy(k, chunk(k)).wait_recv()
        put(update(chunk(k), R, k * rows, R), R, k * rows, R)

    b_copy(last, chunk(last)).wait_recv()
    for p in range(PIECES):
        x_piece(p).wait_recv()
        t = update(pl.ds(last * R + p * piece, piece), piece, last * rows + p * piece, R)
        put(t, piece, last * rows + p * piece, R)

    stat_copies = []
    for i, peer in enumerate((sib, xpeer, diag)):
        copy = pltpu.make_async_remote_copy(src_ref=st.at[me], dst_ref=st.at[me], send_sem=ss_sem.at[i],
                                            recv_sem=sr_sem.at[i], device_id={'tp': peer}, device_id_type=MESH)
        copy.start()
        stat_copies.append(copy)
    for copy in stat_copies:
        copy.wait_recv()
    top = jnp.maximum(jnp.maximum(st[0, 0], st[1, 0]), jnp.maximum(st[2, 0], st[3, 0]))
    norm = jnp.zeros((8, 128), F32)
    hit = jnp.zeros((8, 128), F32)
    for i in range(4):
        norm = norm + st[i, 1] * jnp.exp(st[i, 0] - top)
        hit = hit + st[i, 2]
    m = jnp.max(top, axis=0, keepdims=True)
    for shift in (32, 64):
        m = jnp.maximum(m, pltpu.roll(m, shift, 1))
    norm = jnp.sum(norm * jnp.exp(top - m), axis=0, keepdims=True)
    hit = jnp.sum(hit, axis=0, keepdims=True)
    for shift in (32, 64):
        norm = norm + pltpu.roll(norm, shift, 1)
        hit = hit + pltpu.roll(hit, shift, 1)
    log_norm = m + jnp.log(norm)
    stats_ref[...] = jnp.concatenate([log_norm, hit - log_norm, jnp.zeros((6, 128), F32)], axis=0)
    pick = lax.broadcasted_iota(jnp.int32, (tokens, 128), 0) == lax.broadcasted_iota(jnp.int32, (tokens, 128), 1)
    col = jnp.sum(jnp.where(pick, log_norm, 0.0), axis=1, keepdims=True)
    lncol_ref[...] = jnp.broadcast_to(col, (tokens, 128))

    for copy in stat_copies:
        copy.wait_send()

    @pl.loop(0, last)
    def _(k):
        x_copy(k, chunk(k)).wait_send()

    @pl.loop(0, nf)
    def _(k):
        a_copy(k, chunk(k)).wait_send()
        b_copy(k, chunk(k)).wait_send()

    for p in range(PIECES):
        x_piece(p).wait_send()
    a_copy(nf, tail_rows).wait_send()
    b_copy(nf, tail_rows).wait_send()
    x_copy(nf, tail_rows).wait_send()


def probs_kernel(block, vq, logits_ref, stats_ref, lncol_ref, ln_hbm, tl_hbm, probs_hbm, ln, tl, probs, sem, small_sem):
    tokens = ln.shape[1]
    ln[...] = stats_ref[0:1, :tokens]
    tl[...] = stats_ref[1:2, :tokens]
    copies = [pltpu.make_async_copy(ln, ln_hbm, small_sem.at[0]), pltpu.make_async_copy(tl, tl_hbm, small_sem.at[1])]
    log_norm = lncol_ref[:, 0:1]
    for i, start in enumerate(range(0, vq, block)):
        sl = pl.ds(start, min(block, vq - start))
        probs[:, sl] = jnp.exp(logits_ref[:, sl] - log_norm).astype(BF16)
        if i == 0:
            for copy in copies:
                copy.start()
        copies.append(pltpu.make_async_copy(probs.at[:, sl], probs_hbm.at[:, sl], sem.at[i]))
        copies[-1].start()
    for copy in copies:
        copy.wait()


def solution(mesh):
    def local_scores(hidden, final_gain, table, targets, temperature):
        tokens, hidden_size = hidden.shape
        vocab, width = table.shape
        vq = vocab // 4
        nf = vq // (G * R)
        rt = (vq - nf * G * R) // G
        packed = vq // G
        lanes = (vq + 127) // 128 * 128
        dims = (tokens, hidden_size, width, vq, nf, rt)
        vmem = pl.BlockSpec(memory_space=pltpu.VMEM)
        hbm = pl.BlockSpec(memory_space=pltpu.HBM)
        nsem = nf + PIECES
        logits, stats, lncol = pl.pallas_call(
            functools.partial(scores_kernel, dims),
            out_shape=(pltpu.VMEM((tokens, lanes), F32), pltpu.VMEM((8, 128), F32), pltpu.VMEM((tokens, 128), F32)),
            in_specs=[pl.BlockSpec(memory_space=pltpu.SMEM), hbm, hbm, hbm, hbm],
            out_specs=(vmem, vmem, vmem),
            scratch_shapes=[
                pltpu.VMEM((1, tokens), jnp.int32),
                pltpu.VMEM((tokens, hidden_size), BF16),
                pltpu.VMEM((hidden_size // 128, 128), BF16),
                pltpu.VMEM((hidden_size // 128, 128), F32),
                pltpu.VMEM((G * width, 128), BF16),
                pltpu.VMEM((NBUF, G * R, width), BF16),
                pltpu.VMEM((4, G * rt, width), BF16),
            ] + [pltpu.VMEM((packed, 128), F32)] * 7 + [
                pltpu.VMEM((4, 3, 8, 128), F32),
                pltpu.SemaphoreType.DMA((3,)),
                pltpu.SemaphoreType.DMA((NBUF,)),
                pltpu.SemaphoreType.DMA((4,)),
            ] + [pltpu.SemaphoreType.DMA((nsem,))] * 6 + [
                pltpu.SemaphoreType.DMA((3,)),
                pltpu.SemaphoreType.DMA((3,)),
            ],
            compiler_params=pltpu.CompilerParams(collective_id=0, has_side_effects=True,
                                                 vmem_limit_bytes=50 * 2 ** 20),
        )(temperature.reshape(1, 1), targets.reshape(1, tokens), hidden, final_gain.reshape(hidden_size // 128, 128), table)
        block = 4096
        log_norm, target_logprob, probs = pl.pallas_call(
            functools.partial(probs_kernel, block, vq),
            out_shape=(jax.ShapeDtypeStruct((1, tokens), F32),
                       jax.ShapeDtypeStruct((1, tokens), F32),
                       jax.ShapeDtypeStruct((tokens, vq), BF16)),
            in_specs=[vmem, vmem, vmem],
            out_specs=(hbm, hbm, hbm),
            scratch_shapes=[pltpu.VMEM((1, tokens), F32), pltpu.VMEM((1, tokens), F32),
                            pltpu.VMEM((tokens, vq), BF16),
                            pltpu.SemaphoreType.DMA((pl.cdiv(vq, block),)), pltpu.SemaphoreType.DMA((2,))],
            compiler_params=pltpu.CompilerParams(vmem_limit_bytes=8 * 2 ** 20),
        )(logits, stats, lncol)
        return log_norm.reshape(tokens), target_logprob.reshape(tokens), probs

    return jax.shard_map(local_scores, mesh=mesh,
                         in_specs=(P('dp', None), P(None), P(None, 'tp'), P('dp'), P()),
                         out_specs=(P('dp'), P('dp'), P('dp', 'tp')),
                         check_vma=False)
```

```python
import functools

import jax
import jax.numpy as jnp
from jax import lax
from jax.experimental import pallas as pl
from jax.experimental.pallas import tpu as pltpu
from jax.sharding import PartitionSpec as P

NORM_EPS = 1e-6
MESH = pl.DeviceIdType.MESH
F32 = jnp.float32
BF16 = jnp.bfloat16
G = 4
R = 256
NR = 3
NL = 2
LAG = 2
LATE = 4
PIECES = 2


def scores_kernel(dims, temp_ref, tgt_hbm, hid_hbm, gain_hbm, table, logits_ref, stats_ref, lncol_ref,
                  tgt_ref, hid, gain, gain32, w, ring_r, ring_l, tail, ps, po, ls, lo, ra, rb, rx, acc, st,
                  in_sem, r_sem, l_sem, tail_sem, as_sem, ar_sem, bs_sem, br_sem, xs_sem, xr_sem, ss_sem, sr_sem):
    tokens, hidden_size, width, vq, nf, rt = dims
    me = lax.axis_index('tp')
    x = me // 2
    c = me % 2
    sib = 2 * x + (1 - c)
    xpeer = 2 * (1 - x) + c
    diag = 2 * (1 - x) + (1 - c)
    rows = G * R
    trows = G * rt
    last = nf - 1

    def quarter(chip, half):
        return (2 * chip + ((1 - c) if half == 0 else c)) * vq

    def r_copy(k, half):
        start = pl.multiple_of(quarter(1 - x, half) + k * rows, 64)
        return pltpu.make_async_copy(table.at[pl.ds(start, rows)], ring_r.at[k % NR, half], r_sem.at[k % NR, half])

    def l_copy(k, half):
        start = pl.multiple_of(quarter(x, half) + k * rows, 64)
        return pltpu.make_async_copy(table.at[pl.ds(start, rows)], ring_l.at[k % NL, half], l_sem.at[k % NL, half])

    def tail_copy(i):
        start = pl.multiple_of(quarter((1 - x) if i < 2 else x, i % 2) + nf * rows, 64)
        return pltpu.make_async_copy(table.at[pl.ds(start, trows)], tail.at[i], tail_sem.at[i])

    def chunk(k):
        return pl.ds(pl.multiple_of(k * R, R), R)

    tail_rows = pl.ds(nf * R, rt)

    def remote(src, dst, send, recv, k, sl, dev):
        return pltpu.make_async_remote_copy(src_ref=src.at[sl], dst_ref=dst.at[sl], send_sem=send.at[k],
                                            recv_sem=recv.at[k], device_id={'tp': dev}, device_id_type=MESH)

    def a_copy(k, sl):
        return remote(ps, ra, as_sem, ar_sem, k, sl, sib)

    def b_copy(k, sl):
        return remote(ls, rb, bs_sem, br_sem, k, sl, sib)

    def x_copy(k, sl):
        return remote(po, rx, xs_sem, xr_sem, k, sl, xpeer)

    piece = R // PIECES

    def x_piece(p):
        return x_copy(last if p == 0 else nf + p, pl.ds(last * R + p * piece, piece))

    hid_copy = pltpu.make_async_copy(hid_hbm, hid, in_sem.at[0])
    gain_copy = pltpu.make_async_copy(gain_hbm, gain, in_sem.at[1])
    tgt_copy = pltpu.make_async_copy(tgt_hbm, tgt_ref, in_sem.at[2])
    hid_copy.start()
    gain_copy.start()
    tgt_copy.start()
    tail_copy(0).start()
    tail_copy(1).start()

    barrier = pltpu.get_barrier_semaphore()
    for peer in (sib, xpeer, diag):
        pl.semaphore_signal(barrier, inc=1, device_id={'tp': peer}, device_id_type=MESH)

    hid_copy.wait()
    gain_copy.wait()
    for k in range(NR):
        r_copy(k, 0).start()
        r_copy(k, 1).start()
    tail_copy(2).start()
    tail_copy(3).start()

    hf = hid[...].astype(F32)
    inv = lax.rsqrt(jnp.mean(hf * hf, axis=-1, keepdims=True) + NORM_EPS)
    cols = pl.ds(pl.multiple_of(me * width, 128), width)
    gain32[...] = gain[...].astype(F32)
    scaled = hid[:, cols].astype(F32) * inv
    u = jnp.concatenate([scaled[:, j * 128:(j + 1) * 128] * gain32[pl.ds(me * (width // 128) + j, 1), :]
                         for j in range(width // 128)], axis=1).astype(BF16).astype(F32)
    u_t = jnp.concatenate([u] * G, axis=0).T
    group = lax.broadcasted_iota(jnp.int32, (width, 128), 1) // tokens
    for g in range(G):
        w[g * width:(g + 1) * width, :] = jnp.where(group == g, u_t, 0.0).astype(BF16)
    acc[0] = jnp.full((8, 128), -jnp.inf, F32)
    acc[1] = jnp.zeros((8, 128), F32)
    acc[2] = jnp.zeros((8, 128), F32)
    temp = temp_ref[0, 0]
    lane_group = lax.broadcasted_iota(jnp.int32, (1, 128), 1) // tokens
    tgt_copy.wait()
    tgt = jnp.concatenate([tgt_ref[...]] * G, axis=1) - me * vq

    def packed_dot(views, n):
        total = None
        for g in range(G):
            parts = [view[g * n:(g + 1) * n, :] for view in views]
            lhs = parts[0] if len(parts) == 1 else jnp.concatenate(parts, axis=0)
            part = jnp.dot(lhs, w[g * width:(g + 1) * width, :], preferred_element_type=F32)
            total = part if total is None else total + part
        return total

    def r_dot(k, half, dst):
        r_copy(k, half).wait()
        dst[chunk(k), :] = packed_dot([ring_r.at[k % NR, half]], R)

        @pl.when(k + NR < nf)
        def _():
            r_copy(k + NR, half).start()

    def l_dot(k):
        l_copy(k, 0).wait()
        l_copy(k, 1).wait()
        both = packed_dot([ring_l.at[k % NL, 0], ring_l.at[k % NL, 1]], R)
        ls[chunk(k), :] = both[:R]
        lo[chunk(k), :] = both[R:]

        @pl.when(k + NL < nf)
        def _():
            l_copy(k + NL, 0).start()
            l_copy(k + NL, 1).start()

    def add_sibling(k, sl):
        a_copy(k, sl).wait_recv()
        po[sl, :] = po[sl, :] + ra[sl, :]

    def update(sl, n, base, stride):
        t = (lo[sl, :] + rb[sl, :] + rx[sl, :]) / temp
        t3 = t.reshape(n // 8, 8, 128)
        m_old = acc[0]
        m_new = jnp.maximum(m_old, jnp.max(t3, axis=0))
        acc[0] = m_new
        acc[1] = acc[1] * jnp.exp(m_old - m_new) + jnp.sum(jnp.exp(t3 - m_new), axis=0)
        row = lax.broadcasted_iota(jnp.int32, (n, 128), 0)
        hit = row == (tgt - base - lane_group * stride)
        acc[2] += jnp.sum(jnp.where(hit, t, 0.0).reshape(n // 8, 8, 128), axis=0)
        return t

    def put(t, n, base, stride):
        tt = t.T
        for g in range(G):
            logits_ref[:, pl.ds(pl.multiple_of(base + g * stride, 128), n)] = tt[g * tokens:(g + 1) * tokens, :]

    def finish_tail():
        b_copy(nf, tail_rows).wait_recv()
        x_copy(nf, tail_rows).wait_recv()
        t = update(tail_rows, rt, nf * rows, rt)
        tt = jnp.concatenate([t, jnp.zeros((128 - rt, 128), F32)], axis=0).T
        parts = [tt[g * tokens:(g + 1) * tokens, :] for g in range(G)]
        lane = lax.broadcasted_iota(jnp.int32, (tokens, 128), 1)
        for i in range((G * rt + 127) // 128):
            tile = jnp.zeros((tokens, 128), F32)
            for g in range(G):
                off = g * rt - i * 128
                if off <= -rt or off >= 128:
                    continue
                moved = pltpu.roll(parts[g], off % 128, 1) if off % 128 else parts[g]
                tile = jnp.where((lane >= off) & (lane < off + rt), moved, tile)
            logits_ref[:, nf * rows + i * 128:nf * rows + (i + 1) * 128] = tile
        a_copy(nf, tail_rows).wait_send()
        b_copy(nf, tail_rows).wait_send()
        x_copy(nf, tail_rows).wait_send()

    tail_copy(0).wait()
    ps[tail_rows, :] = packed_dot([tail.at[0]], rt)
    tail_copy(1).wait()
    po[tail_rows, :] = packed_dot([tail.at[1]], rt)
    pl.semaphore_wait(barrier, 3)
    a_copy(nf, tail_rows).start()

    @pl.loop(0, nf + LATE - 1)
    def _(j):
        @pl.when(j < nf)
        def _():
            r_dot(j, 0, ps)
            a_copy(j, chunk(j)).start()

        @pl.when(j == 0)
        def _():
            add_sibling(nf, tail_rows)
            x_copy(nf, tail_rows).start()

        @pl.when(jnp.logical_and(j > 0, j <= nf))
        def _():
            add_sibling(j - 1, chunk(j - 1))

        @pl.when(j == 1)
        def _():
            x_copy(j - 1, chunk(j - 1)).start()

        @pl.when(j < nf)
        def _():
            r_dot(j, 1, po)

        @pl.when(jnp.logical_and(j > 1, j < nf))
        def _():
            x_copy(j - 1, chunk(j - 1)).start()

        @pl.when(j < NL)
        def _():
            l_copy(j, 0).start()
            l_copy(j, 1).start()

        @pl.when(jnp.logical_and(j > LAG, j <= nf + LAG))
        def _():
            b_copy(j - LAG - 1, chunk(j - LAG - 1)).start()

        @pl.when(jnp.logical_and(j >= LAG, j < nf + LAG))
        def _():
            l_dot(j - LAG)

        @pl.when(j == nf)
        def _():
            for p in range(PIECES):
                x_piece(p).start()

        @pl.when(j == 4)
        def _():
            tail_copy(2).wait()
            tail_copy(3).wait()
            both = packed_dot([tail.at[2], tail.at[3]], rt)
            ls[tail_rows, :] = both[:rt]
            lo[tail_rows, :] = both[rt:]

        @pl.when(j == 5)
        def _():
            b_copy(nf, tail_rows).start()

        @pl.when(j == 8)
        def _():
            finish_tail()

        @pl.when(j >= LATE)
        def _():
            k = j - LATE
            b_copy(k, chunk(k)).wait_recv()
            x_copy(k, chunk(k)).wait_recv()
            put(update(chunk(k), R, k * rows, R), R, k * rows, R)
            a_copy(k, chunk(k)).wait_send()
            b_copy(k, chunk(k)).wait_send()

            @pl.when(k > 0)
            def _():
                x_copy(k - 1, chunk(k - 1)).wait_send()

    x_copy(last - 1, chunk(last - 1)).wait_send()
    a_copy(last, chunk(last)).wait_send()
    b_copy(last, chunk(last)).wait_send()
    b_copy(last, chunk(last)).wait_recv()
    for p in range(PIECES):
        x_piece(p).wait_recv()
        t = update(pl.ds(last * R + p * piece, piece), piece, last * rows + p * piece, R)
        put(t, piece, last * rows + p * piece, R)

    m = jnp.max(acc[0], axis=0, keepdims=True)
    norm = jnp.sum(acc[1] * jnp.exp(acc[0] - m), axis=0, keepdims=True)
    hit = jnp.sum(acc[2], axis=0, keepdims=True)
    st[me] = jnp.concatenate([m, norm, hit, jnp.zeros((5, 128), F32)], axis=0)
    for p in range(PIECES):
        x_piece(p).wait_send()
    stat_copies = []
    for i, peer in enumerate((xpeer, diag, sib)):
        copy = pltpu.make_async_remote_copy(src_ref=st.at[me], dst_ref=st.at[me], send_sem=ss_sem.at[i],
                                            recv_sem=sr_sem.at[i], device_id={'tp': peer}, device_id_type=MESH)
        copy.start()
        stat_copies.append(copy)
    for copy in stat_copies:
        copy.wait_send()
    for copy in stat_copies:
        copy.wait_recv()
    ms, ns, hit = [], [], jnp.zeros((1, 128), F32)
    for i in range(4):
        hit = hit + st[i, 2:3, :]
        for shift in range(0, G * tokens, tokens):
            ms.append(pltpu.roll(st[i, 0:1, :], shift, 1) if shift else st[i, 0:1, :])
            ns.append(pltpu.roll(st[i, 1:2, :], shift, 1) if shift else st[i, 1:2, :])
    hit = sum(pltpu.roll(hit, shift, 1) for shift in range(tokens, G * tokens, tokens)) + hit
    top = functools.reduce(jnp.maximum, ms)
    norm = sum(n * jnp.exp(m - top) for n, m in zip(ns, ms))
    log_norm = top + jnp.log(norm)
    stats_ref[...] = jnp.concatenate([log_norm, hit - log_norm, jnp.zeros((6, 128), F32)], axis=0)
    pick = lax.broadcasted_iota(jnp.int32, (tokens, 128), 0) == lax.broadcasted_iota(jnp.int32, (tokens, 128), 1)
    col = jnp.sum(jnp.where(pick, log_norm, 0.0), axis=1, keepdims=True)
    lncol_ref[...] = jnp.broadcast_to(col, (tokens, 128))


def probs_kernel(block, vq, logits_ref, stats_ref, lncol_ref, ln_hbm, tl_hbm, probs_hbm, ln, tl, probs, sem, small_sem):
    tokens = ln.shape[1]
    ln[...] = stats_ref[0:1, :tokens]
    tl[...] = stats_ref[1:2, :tokens]
    copies = [pltpu.make_async_copy(ln, ln_hbm, small_sem.at[0]), pltpu.make_async_copy(tl, tl_hbm, small_sem.at[1])]
    log_norm = lncol_ref[:, 0:1]
    for i, start in enumerate(range(0, vq, block)):
        sl = pl.ds(start, min(block, vq - start))
        probs[:, sl] = jnp.exp(logits_ref[:, sl] - log_norm).astype(BF16)
        if i == 0:
            for copy in copies:
                copy.start()
        copies.append(pltpu.make_async_copy(probs.at[:, sl], probs_hbm.at[:, sl], sem.at[i]))
        copies[-1].start()
    for copy in copies:
        copy.wait()


def solution(mesh):
    def local_scores(hidden, final_gain, table, targets, temperature):
        tokens, hidden_size = hidden.shape
        vocab, width = table.shape
        vq = vocab // 4
        nf = vq // (G * R)
        rt = (vq - nf * G * R) // G
        packed = vq // G
        lanes = (vq + 127) // 128 * 128
        dims = (tokens, hidden_size, width, vq, nf, rt)
        vmem = pl.BlockSpec(memory_space=pltpu.VMEM)
        hbm = pl.BlockSpec(memory_space=pltpu.HBM)
        nsem = nf + PIECES
        logits, stats, lncol = pl.pallas_call(
            functools.partial(scores_kernel, dims),
            out_shape=(pltpu.VMEM((tokens, lanes), F32), pltpu.VMEM((8, 128), F32), pltpu.VMEM((tokens, 128), F32)),
            in_specs=[pl.BlockSpec(memory_space=pltpu.SMEM), hbm, hbm, hbm, hbm],
            out_specs=(vmem, vmem, vmem),
            scratch_shapes=[
                pltpu.VMEM((1, tokens), jnp.int32),
                pltpu.VMEM((tokens, hidden_size), BF16),
                pltpu.VMEM((hidden_size // 128, 128), BF16),
                pltpu.VMEM((hidden_size // 128, 128), F32),
                pltpu.VMEM((G * width, 128), BF16),
                pltpu.VMEM((NR, 2, G * R, width), BF16),
                pltpu.VMEM((NL, 2, G * R, width), BF16),
                pltpu.VMEM((4, G * rt, width), BF16),
            ] + [pltpu.VMEM((packed, 128), F32)] * 7 + [
                pltpu.VMEM((3, 8, 128), F32),
                pltpu.VMEM((4, 8, 128), F32),
                pltpu.SemaphoreType.DMA((3,)),
                pltpu.SemaphoreType.DMA((NR, 2)),
                pltpu.SemaphoreType.DMA((NL, 2)),
                pltpu.SemaphoreType.DMA((4,)),
            ] + [pltpu.SemaphoreType.DMA((nsem,))] * 6 + [
                pltpu.SemaphoreType.DMA((3,)),
                pltpu.SemaphoreType.DMA((3,)),
            ],
            compiler_params=pltpu.CompilerParams(collective_id=0, has_side_effects=True,
                                                 vmem_limit_bytes=54 * 2 ** 20),
        )(temperature.reshape(1, 1), targets.reshape(1, tokens), hidden, final_gain.reshape(hidden_size // 128, 128), table)
        block = 4096
        log_norm, target_logprob, probs = pl.pallas_call(
            functools.partial(probs_kernel, block, vq),
            out_shape=(jax.ShapeDtypeStruct((1, tokens), F32),
                       jax.ShapeDtypeStruct((1, tokens), F32),
                       jax.ShapeDtypeStruct((tokens, vq), BF16)),
            in_specs=[vmem, vmem, vmem],
            out_specs=(hbm, hbm, hbm),
            scratch_shapes=[pltpu.VMEM((1, tokens), F32), pltpu.VMEM((1, tokens), F32),
                            pltpu.VMEM((tokens, vq), BF16),
                            pltpu.SemaphoreType.DMA((pl.cdiv(vq, block),)), pltpu.SemaphoreType.DMA((2,))],
            compiler_params=pltpu.CompilerParams(vmem_limit_bytes=8 * 2 ** 20),
        )(logits, stats, lncol)
        return log_norm.reshape(tokens), target_logprob.reshape(tokens), probs

    return jax.shard_map(local_scores, mesh=mesh,
                         in_specs=(P('dp', None), P(None), P(None, 'tp'), P('dp'), P()),
                         out_specs=(P('dp'), P('dp'), P('dp', 'tp')),
                         check_vma=False)
```

```python
import functools

import jax
import jax.numpy as jnp
from jax import lax
from jax.experimental import pallas as pl
from jax.experimental.pallas import tpu as pltpu
from jax.sharding import PartitionSpec as P

NORM_EPS = 1e-6
MESH = pl.DeviceIdType.MESH
F32 = jnp.float32
BF16 = jnp.bfloat16
G = 4
R = 256
NR = 3
NL = 2
LAG = 2
LATE = 4
NA, NB, NS, NX = 5, 5, 5, 2 * LATE


def scores_kernel(dims, temp_ref, tgt_hbm, hid_hbm, gain_hbm, table, logits_ref, stats_ref, scale_ref,
                  tgt_ref, hid, gain, gain32, w, ring_r, ring_l, tail, ps, po, ls, lo, ra, rb, rx, rx2, acc, st,
                  in_sem, r_sem, l_sem, tail_sem, as_sem, ar_sem, bs_sem, br_sem, xs_sem, xr_sem, one_sem, ss_sem, sr_sem):
    tokens, hidden_size, width, vq, nf, rt = dims
    me = lax.axis_index('tp')
    x = me // 2
    c = me % 2
    sib = 2 * x + (1 - c)
    xpeer = 2 * (1 - x) + c
    diag = 2 * (1 - x) + (1 - c)
    rows = G * R
    trows = G * rt
    last = nf - 1

    def quarter(chip, half):
        return (2 * chip + ((1 - c) if half == 0 else c)) * vq

    def r_copy(k, half):
        start = pl.multiple_of(quarter(1 - x, half) + k * rows, 64)
        return pltpu.make_async_copy(table.at[pl.ds(start, rows)], ring_r.at[k % NR, half], r_sem.at[k % NR, half])

    def l_copy(k, half):
        start = pl.multiple_of(quarter(x, half) + k * rows, 64)
        return pltpu.make_async_copy(table.at[pl.ds(start, rows)], ring_l.at[k % NL, half], l_sem.at[k % NL, half])

    def tail_copy(i):
        start = pl.multiple_of(quarter((1 - x) if i < 2 else x, i % 2) + nf * rows, 64)
        return pltpu.make_async_copy(table.at[pl.ds(start, trows)], tail.at[i], tail_sem.at[i])

    def chunk(k):
        return pl.ds(pl.multiple_of(k * R, R), R)

    tail_rows = pl.ds(nf * R, rt)

    def remote(src, dst, send, recv, dev):
        return pltpu.make_async_remote_copy(src_ref=src, dst_ref=dst, send_sem=send, recv_sem=recv,
                                            device_id={'tp': dev}, device_id_type=MESH)

    def a_copy(k):
        sl = chunk(k)
        return remote(ps.at[sl], ra.at[sl], as_sem.at[k % 2], ar_sem.at[k % NA], sib)

    def b_copy(k):
        sl = chunk(k)
        return remote(ls.at[sl], rb.at[sl], bs_sem.at[k % 2], br_sem.at[k % NB], sib)

    def x_copy(k):
        sl = chunk(k)
        return remote(po.at[sl], rx.at[sl], xs_sem.at[k % NS], xr_sem.at[k % NX], xpeer)

    def b_tail():
        return remote(ls.at[tail_rows], rb.at[tail_rows], one_sem.at[0], one_sem.at[1], sib)

    def x_tail():
        return remote(po.at[tail_rows], rx.at[tail_rows], one_sem.at[2], one_sem.at[3], xpeer)

    def x2_tail():
        return remote(ps.at[tail_rows], rx2, one_sem.at[4], one_sem.at[5], diag)

    piece = R // 2

    def x_piece(p):
        sl = pl.ds(last * R + p * piece, piece)
        send, recv = (one_sem.at[6], one_sem.at[7]) if p else (xs_sem.at[last % NS], xr_sem.at[last % NX])
        return remote(po.at[sl], rx.at[sl], send, recv, xpeer)

    hid_copy = pltpu.make_async_copy(hid_hbm, hid, in_sem.at[0])
    gain_copy = pltpu.make_async_copy(gain_hbm, gain, in_sem.at[1])
    tgt_copy = pltpu.make_async_copy(tgt_hbm, tgt_ref, in_sem.at[2])
    hid_copy.start()
    gain_copy.start()
    tgt_copy.start()
    tail_copy(0).start()
    tail_copy(1).start()

    barrier = pltpu.get_barrier_semaphore()
    for peer in (sib, xpeer, diag):
        pl.semaphore_signal(barrier, inc=1, device_id={'tp': peer}, device_id_type=MESH)

    hid_copy.wait()
    gain_copy.wait()
    for k in range(NR):
        r_copy(k, 0).start()
        r_copy(k, 1).start()
    tail_copy(2).start()
    tail_copy(3).start()

    hf = hid[...].astype(F32)
    inv = lax.rsqrt(jnp.mean(hf * hf, axis=-1, keepdims=True) + NORM_EPS)
    cols = pl.ds(pl.multiple_of(me * width, 128), width)
    gain32[...] = gain[...].astype(F32)
    scaled = hid[:, cols].astype(F32) * inv
    u = jnp.concatenate([scaled[:, j * 128:(j + 1) * 128] * gain32[pl.ds(me * (width // 128) + j, 1), :]
                         for j in range(width // 128)], axis=1).astype(BF16).astype(F32)
    u_t = jnp.concatenate([u] * G, axis=0).T
    group = lax.broadcasted_iota(jnp.int32, (width, 128), 1) // tokens
    for g in range(G):
        w[g * width:(g + 1) * width, :] = jnp.where(group == g, u_t, 0.0).astype(BF16)
    acc[0] = jnp.full((8, 128), -jnp.inf, F32)
    acc[1] = jnp.zeros((8, 128), F32)
    acc[2] = jnp.zeros((8, 128), F32)
    temp = temp_ref[0, 0]
    lane_group = lax.broadcasted_iota(jnp.int32, (1, 128), 1) // tokens
    tgt_copy.wait()
    tgt = jnp.concatenate([tgt_ref[...]] * G, axis=1) - me * vq

    def packed_dot(views, n):
        total = None
        for g in range(G):
            parts = [view[g * n:(g + 1) * n, :] for view in views]
            lhs = parts[0] if len(parts) == 1 else jnp.concatenate(parts, axis=0)
            part = jnp.dot(lhs, w[g * width:(g + 1) * width, :], preferred_element_type=F32)
            total = part if total is None else total + part
        return total

    def r_dot(k, half, dst):
        r_copy(k, half).wait()
        dst[chunk(k), :] = packed_dot([ring_r.at[k % NR, half]], R)

        @pl.when(k + NR < nf)
        def _():
            r_copy(k + NR, half).start()

    def l_dot(k):
        l_copy(k, 0).wait()
        l_copy(k, 1).wait()
        both = packed_dot([ring_l.at[k % NL, 0], ring_l.at[k % NL, 1]], R)
        ls[chunk(k), :] = both[:R]
        lo[chunk(k), :] = both[R:]

        @pl.when(k + NL < nf)
        def _():
            l_copy(k + NL, 0).start()
            l_copy(k + NL, 1).start()

    def add_sibling(k):
        sl = chunk(k)
        a_copy(k).wait_recv()
        po[sl, :] = po[sl, :] + ra[sl, :]

    def update(sl, n, base, stride, crossed=None):
        z = lo[sl, :] + rb[sl, :] + rx[sl, :]
        t = (z if crossed is None else z + crossed) / temp
        t3 = t.reshape(n // 8, 8, 128)
        m_old = acc[0]
        m_new = jnp.maximum(m_old, jnp.max(t3, axis=0))
        acc[0] = m_new
        acc[1] = acc[1] * jnp.exp(m_old - m_new) + jnp.sum(jnp.exp(t3 - m_new), axis=0)
        row = lax.broadcasted_iota(jnp.int32, (n, 128), 0)
        hit = row == (tgt - base - lane_group * stride)
        acc[2] += jnp.sum(jnp.where(hit, t, 0.0).reshape(n // 8, 8, 128), axis=0)
        return t

    def put(t, n, base, stride):
        tt = t.T
        for g in range(G):
            logits_ref[:, pl.ds(pl.multiple_of(base + g * stride, 128), n)] = tt[g * tokens:(g + 1) * tokens, :]

    def finish_tail():
        b_tail().wait_recv()
        x_tail().wait_recv()
        x2_tail().wait_recv()
        t = update(tail_rows, rt, nf * rows, rt, rx2[...])
        tt = jnp.concatenate([t, jnp.zeros((128 - rt, 128), F32)], axis=0).T
        parts = [tt[g * tokens:(g + 1) * tokens, :] for g in range(G)]
        lane = lax.broadcasted_iota(jnp.int32, (tokens, 128), 1)
        for i in range((G * rt + 127) // 128):
            tile = jnp.zeros((tokens, 128), F32)
            for g in range(G):
                off = g * rt - i * 128
                if off <= -rt or off >= 128:
                    continue
                moved = pltpu.roll(parts[g], off % 128, 1) if off % 128 else parts[g]
                tile = jnp.where((lane >= off) & (lane < off + rt), moved, tile)
            logits_ref[:, nf * rows + i * 128:nf * rows + (i + 1) * 128] = tile
        b_tail().wait_send()
        x_tail().wait_send()
        x2_tail().wait_send()

    tail_copy(0).wait()
    ps[tail_rows, :] = packed_dot([tail.at[0]], rt)
    tail_copy(1).wait()
    po[tail_rows, :] = packed_dot([tail.at[1]], rt)
    pl.semaphore_wait(barrier, 3)
    x_tail().start()
    x2_tail().start()

    @pl.loop(0, nf + LATE - 1)
    def _(j):
        @pl.when(j < nf)
        def _():
            r_dot(j, 0, ps)

            @pl.when(j >= 2)
            def _():
                a_copy(j - 2).wait_send()

            a_copy(j).start()

        @pl.when(jnp.logical_and(j > 0, j <= nf))
        def _():
            add_sibling(j - 1)

        @pl.when(j == 1)
        def _():
            x_copy(j - 1).start()

        @pl.when(j < nf)
        def _():
            r_dot(j, 1, po)

        @pl.when(jnp.logical_and(j > 1, j < nf))
        def _():
            x_copy(j - 1).start()

        @pl.when(j < NL)
        def _():
            l_copy(j, 0).start()
            l_copy(j, 1).start()

        @pl.when(jnp.logical_and(j > LAG, j <= nf + LAG))
        def _():
            k = j - LAG - 1

            @pl.when(k >= 2)
            def _():
                b_copy(k - 2).wait_send()

            b_copy(k).start()

        @pl.when(jnp.logical_and(j >= LAG, j < nf + LAG))
        def _():
            l_dot(j - LAG)

        @pl.when(j == nf)
        def _():
            for p in range(2):
                x_piece(p).start()

        @pl.when(j == 4)
        def _():
            tail_copy(2).wait()
            tail_copy(3).wait()
            both = packed_dot([tail.at[2], tail.at[3]], rt)
            ls[tail_rows, :] = both[:rt]
            lo[tail_rows, :] = both[rt:]

        @pl.when(j == 5)
        def _():
            b_tail().start()

        @pl.when(j == 8)
        def _():
            finish_tail()

        @pl.when(j >= LATE)
        def _():
            k = j - LATE
            b_copy(k).wait_recv()
            x_copy(k).wait_recv()
            put(update(chunk(k), R, k * rows, R), R, k * rows, R)

            @pl.when(k > 0)
            def _():
                x_copy(k - 1).wait_send()

    for k in (last - 1, last):
        a_copy(k).wait_send()
        b_copy(k).wait_send()
    x_copy(last - 1).wait_send()
    b_copy(last).wait_recv()
    for p in range(2):
        x_piece(p).wait_recv()
        t = update(pl.ds(last * R + p * piece, piece), piece, last * rows + p * piece, R)
        put(t, piece, last * rows + p * piece, R)

    m = jnp.max(acc[0], axis=0, keepdims=True)
    norm = jnp.sum(acc[1] * jnp.exp(acc[0] - m), axis=0, keepdims=True)
    hit = jnp.sum(acc[2], axis=0, keepdims=True)
    st[me] = jnp.concatenate([m, norm, hit, jnp.zeros((5, 128), F32)], axis=0)
    for p in range(2):
        x_piece(p).wait_send()
    stat_copies = []
    for i, peer in enumerate((xpeer, diag, sib)):
        copy = pltpu.make_async_remote_copy(src_ref=st.at[me], dst_ref=st.at[me], send_sem=ss_sem.at[i],
                                            recv_sem=sr_sem.at[i], device_id={'tp': peer}, device_id_type=MESH)
        copy.start()
        stat_copies.append(copy)
    pick = lax.broadcasted_iota(jnp.int32, (tokens, 128), 0) == lax.broadcasted_iota(jnp.int32, (tokens, 128), 1)

    def column(row):
        return jnp.sum(jnp.where(pick, row, 0.0), axis=1, keepdims=True)

    own = functools.reduce(jnp.maximum, [pltpu.roll(m, shift, 1) for shift in range(tokens, G * tokens, tokens)], m)
    own_col = column(own)

    @pl.loop(0, nf)
    def _(k):
        sl = pl.ds(pl.multiple_of(k * rows, 128), rows)
        logits_ref[:, sl] = jnp.exp(logits_ref[:, sl] - own_col)

    sl = pl.ds(nf * rows, logits_ref.shape[1] - nf * rows)
    logits_ref[:, sl] = jnp.exp(logits_ref[:, sl] - own_col)
    for copy in stat_copies:
        copy.wait_send()
    for copy in stat_copies:
        copy.wait_recv()
    ms, ns, hit = [], [], jnp.zeros((1, 128), F32)
    for i in range(4):
        hit = hit + st[i, 2:3, :]
        for shift in range(0, G * tokens, tokens):
            ms.append(pltpu.roll(st[i, 0:1, :], shift, 1) if shift else st[i, 0:1, :])
            ns.append(pltpu.roll(st[i, 1:2, :], shift, 1) if shift else st[i, 1:2, :])
    hit = sum(pltpu.roll(hit, shift, 1) for shift in range(tokens, G * tokens, tokens)) + hit
    top = functools.reduce(jnp.maximum, ms)
    norm = sum(n * jnp.exp(m - top) for n, m in zip(ns, ms))
    log_norm = top + jnp.log(norm)
    stats_ref[...] = jnp.concatenate([log_norm, hit - log_norm, jnp.zeros((6, 128), F32)], axis=0)
    scale_ref[...] = jnp.broadcast_to(column(jnp.exp(own - log_norm)), (tokens, 128))


def probs_kernel(block, vq, exp_ref, stats_ref, scale_ref, ln_hbm, tl_hbm, probs_hbm, ln, tl, probs, sem, small_sem):
    tokens = ln.shape[1]
    ln[...] = stats_ref[0:1, :tokens]
    tl[...] = stats_ref[1:2, :tokens]
    copies = [pltpu.make_async_copy(ln, ln_hbm, small_sem.at[0]), pltpu.make_async_copy(tl, tl_hbm, small_sem.at[1])]
    scale = scale_ref[:, 0:1]
    for i, start in enumerate(range(0, vq, block)):
        sl = pl.ds(start, min(block, vq - start))
        probs[:, sl] = (exp_ref[:, sl] * scale).astype(BF16)
        if i == 0:
            for copy in copies:
                copy.start()
        pltpu.make_async_copy(probs.at[:, sl], probs_hbm.at[:, sl], sem.at[0]).start()
    copies.append(pltpu.make_async_copy(probs, probs_hbm, sem.at[0]))
    for copy in copies:
        copy.wait()


def solution(mesh):
    def local_scores(hidden, final_gain, table, targets, temperature):
        tokens, hidden_size = hidden.shape
        vocab, width = table.shape
        vq = vocab // 4
        nf = vq // (G * R)
        rt = (vq - nf * G * R) // G
        packed = vq // G
        lanes = (vq + 127) // 128 * 128
        dims = (tokens, hidden_size, width, vq, nf, rt)
        vmem = pl.BlockSpec(memory_space=pltpu.VMEM)
        hbm = pl.BlockSpec(memory_space=pltpu.HBM)
        exps, stats, scale = pl.pallas_call(
            functools.partial(scores_kernel, dims),
            out_shape=(pltpu.VMEM((tokens, lanes), F32), pltpu.VMEM((8, 128), F32), pltpu.VMEM((tokens, 128), F32)),
            in_specs=[pl.BlockSpec(memory_space=pltpu.SMEM), hbm, hbm, hbm, hbm],
            out_specs=(vmem, vmem, vmem),
            scratch_shapes=[
                pltpu.VMEM((1, tokens), jnp.int32),
                pltpu.VMEM((tokens, hidden_size), BF16),
                pltpu.VMEM((hidden_size // 128, 128), BF16),
                pltpu.VMEM((hidden_size // 128, 128), F32),
                pltpu.VMEM((G * width, 128), BF16),
                pltpu.VMEM((NR, 2, G * R, width), BF16),
                pltpu.VMEM((NL, 2, G * R, width), BF16),
                pltpu.VMEM((4, G * rt, width), BF16),
            ] + [pltpu.VMEM((packed, 128), F32)] * 7 + [
                pltpu.VMEM((rt, 128), F32),
                pltpu.VMEM((3, 8, 128), F32),
                pltpu.VMEM((4, 8, 128), F32),
                pltpu.SemaphoreType.DMA((3,)),
                pltpu.SemaphoreType.DMA((NR, 2)),
                pltpu.SemaphoreType.DMA((NL, 2)),
                pltpu.SemaphoreType.DMA((4,)),
            ] + [pltpu.SemaphoreType.DMA((n,)) for n in (2, NA, 2, NB, NS, NX, 8)] + [
                pltpu.SemaphoreType.DMA((3,)),
                pltpu.SemaphoreType.DMA((3,)),
            ],
            compiler_params=pltpu.CompilerParams(collective_id=0, has_side_effects=True,
                                                 vmem_limit_bytes=54 * 2 ** 20),
        )(temperature.reshape(1, 1), targets.reshape(1, tokens), hidden, final_gain.reshape(hidden_size // 128, 128), table)
        block = 4096
        log_norm, target_logprob, probs = pl.pallas_call(
            functools.partial(probs_kernel, block, vq),
            out_shape=(jax.ShapeDtypeStruct((1, tokens), F32),
                       jax.ShapeDtypeStruct((1, tokens), F32),
                       jax.ShapeDtypeStruct((tokens, vq), BF16)),
            in_specs=[vmem, vmem, vmem],
            out_specs=(hbm, hbm, hbm),
            scratch_shapes=[pltpu.VMEM((1, tokens), F32), pltpu.VMEM((1, tokens), F32),
                            pltpu.VMEM((tokens, vq), BF16),
                            pltpu.SemaphoreType.DMA((1,)), pltpu.SemaphoreType.DMA((2,))],
            compiler_params=pltpu.CompilerParams(vmem_limit_bytes=8 * 2 ** 20),
        )(exps, stats, scale)
        return log_norm.reshape(tokens), target_logprob.reshape(tokens), probs

    return jax.shard_map(local_scores, mesh=mesh,
                         in_specs=(P('dp', None), P(None), P(None, 'tp'), P('dp'), P()),
                         out_specs=(P('dp'), P('dp'), P('dp', 'tp')),
                         check_vma=False)
```

```python
import functools

import jax
import jax.numpy as jnp
from jax import lax
from jax.experimental import pallas as pl
from jax.experimental.pallas import tpu as pltpu
from jax.sharding import PartitionSpec as P

NORM_EPS = 1e-6
MESH = pl.DeviceIdType.MESH
F32 = jnp.float32
BF16 = jnp.bfloat16
G = 4
R = 256
NR = 2
NL = 2
LAG = 2
LATE = 4
NA, NB, NS, NX = 5, 5, 5, 2 * LATE


def scores_kernel(dims, temp_ref, tgt_hbm, hid_hbm, gain_hbm, table, logits_ref, stats_ref, scale_ref,
                  tgt_ref, hid, gain, gain32, w, ring_r, ring_l, tail, ps, po, ls, lo, ra, rb, rx, rx2, acc, st,
                  in_sem, r_sem, l_sem, as_sem, ar_sem, bs_sem, br_sem, xs_sem, xr_sem, one_sem, ss_sem, sr_sem):
    tokens, hidden_size, width, vq, nf, rt = dims
    me = lax.axis_index('tp')
    x = me // 2
    c = me % 2
    sib = 2 * x + (1 - c)
    xpeer = 2 * (1 - x) + c
    diag = 2 * (1 - x) + (1 - c)
    rows = G * R
    trows = G * rt
    last = nf - 1

    def quarter(chip, half):
        return (2 * chip + ((1 - c) if half == 0 else c)) * vq

    def r_copy(k, half):
        start = pl.multiple_of(quarter(1 - x, half) + k * rows, 64)
        return pltpu.make_async_copy(table.at[pl.ds(start, rows)], ring_r.at[k % NR, half], r_sem.at[k % NR, half])

    def l_copy(k, half):
        start = pl.multiple_of(quarter(x, half) + k * rows, 64)
        return pltpu.make_async_copy(table.at[pl.ds(start, rows)], ring_l.at[k % NL, half], l_sem.at[k % NL, half])

    def tail_copy(i):
        start = pl.multiple_of(quarter((1 - x) if i < 2 else x, i % 2) + nf * rows, 64)
        return pltpu.make_async_copy(table.at[pl.ds(start, trows)], tail.at[i], (l_sem.at[0, i] if i < 2 else in_sem.at[i - 2]))

    def chunk(k):
        return pl.ds(pl.multiple_of(k * R, R), R)

    tail_rows = pl.ds(nf * R, rt)

    def remote(src, dst, send, recv, dev):
        return pltpu.make_async_remote_copy(src_ref=src, dst_ref=dst, send_sem=send, recv_sem=recv,
                                            device_id={'tp': dev}, device_id_type=MESH)

    def a_copy(k):
        sl = chunk(k)
        return remote(ps.at[sl], ra.at[sl], as_sem.at[k % 2], ar_sem.at[k % NA], sib)

    def b_copy(k):
        sl = chunk(k)
        return remote(ls.at[sl], rb.at[sl], bs_sem.at[k % 2], br_sem.at[k % NB], sib)

    def x_copy(k):
        sl = chunk(k)
        return remote(po.at[sl], rx.at[sl], xs_sem.at[k % NS], xr_sem.at[k % NX], xpeer)

    def b_tail():
        return remote(ls.at[tail_rows], rb.at[tail_rows], one_sem.at[0], one_sem.at[1], sib)

    def x_tail():
        return remote(po.at[tail_rows], rx.at[tail_rows], one_sem.at[2], one_sem.at[3], xpeer)

    def x2_tail():
        return remote(ps.at[tail_rows], rx2, one_sem.at[4], one_sem.at[5], diag)

    piece = R // 2

    def x_piece(p):
        sl = pl.ds(last * R + p * piece, piece)
        send, recv = (one_sem.at[6], one_sem.at[7]) if p else (xs_sem.at[last % NS], xr_sem.at[last % NX])
        return remote(po.at[sl], rx.at[sl], send, recv, xpeer)

    hid_copy = pltpu.make_async_copy(hid_hbm, hid, in_sem.at[0])
    gain_copy = pltpu.make_async_copy(gain_hbm, gain, in_sem.at[1])
    tgt_copy = pltpu.make_async_copy(tgt_hbm, tgt_ref, in_sem.at[2])
    hid_copy.start()
    gain_copy.start()
    tgt_copy.start()
    tail_copy(0).start()
    tail_copy(1).start()

    barrier = pltpu.get_barrier_semaphore()
    for peer in (sib, xpeer, diag):
        pl.semaphore_signal(barrier, inc=1, device_id={'tp': peer}, device_id_type=MESH)

    hid_copy.wait()
    gain_copy.wait()
    for k in range(NR):
        r_copy(k, 0).start()
        r_copy(k, 1).start()
    tail_copy(2).start()
    tail_copy(3).start()

    hf = hid[...].astype(F32)
    inv = lax.rsqrt(jnp.mean(hf * hf, axis=-1, keepdims=True) + NORM_EPS)
    cols = pl.ds(pl.multiple_of(me * width, 128), width)
    gain32[...] = gain[...].astype(F32)
    scaled = hid[:, cols].astype(F32) * inv
    u = jnp.concatenate([scaled[:, j * 128:(j + 1) * 128] * gain32[pl.ds(me * (width // 128) + j, 1), :]
                         for j in range(width // 128)], axis=1).astype(BF16).astype(F32)
    u_t = jnp.concatenate([u] * G, axis=0).T
    group = lax.broadcasted_iota(jnp.int32, (width, 128), 1) // tokens
    for g in range(G):
        w[g * width:(g + 1) * width, :] = jnp.where(group == g, u_t, 0.0).astype(BF16)
    acc[0] = jnp.full((8, 128), -jnp.inf, F32)
    acc[1] = jnp.zeros((8, 128), F32)
    acc[2] = jnp.zeros((8, 128), F32)
    temp = temp_ref[0, 0]
    lane_group = lax.broadcasted_iota(jnp.int32, (1, 128), 1) // tokens
    tgt_copy.wait()
    tgt = jnp.concatenate([tgt_ref[...]] * G, axis=1) - me * vq

    def packed_dot(views, n):
        total = None
        for g in range(G):
            parts = [view[g * n:(g + 1) * n, :] for view in views]
            lhs = parts[0] if len(parts) == 1 else jnp.concatenate(parts, axis=0)
            part = jnp.dot(lhs, w[g * width:(g + 1) * width, :], preferred_element_type=F32)
            total = part if total is None else total + part
        return total

    def r_dot(k, half, dst):
        r_copy(k, half).wait()
        dst[chunk(k), :] = packed_dot([ring_r.at[k % NR, half]], R)

        @pl.when(k + NR < nf)
        def _():
            r_copy(k + NR, half).start()

    def l_dot(k):
        l_copy(k, 0).wait()
        l_copy(k, 1).wait()
        both = packed_dot([ring_l.at[k % NL, 0], ring_l.at[k % NL, 1]], R)
        ls[chunk(k), :] = both[:R]
        lo[chunk(k), :] = both[R:]

        @pl.when(k + NL < nf)
        def _():
            l_copy(k + NL, 0).start()
            l_copy(k + NL, 1).start()

    def add_sibling(k):
        sl = chunk(k)
        a_copy(k).wait_recv()
        po[sl, :] = po[sl, :] + ra[sl, :]

    def update(sl, n, base, stride, crossed=None):
        z = lo[sl, :] + rb[sl, :] + rx[sl, :]
        t = (z if crossed is None else z + crossed) / temp
        t3 = t.reshape(n // 8, 8, 128)
        m_old = acc[0]
        m_new = jnp.maximum(m_old, jnp.max(t3, axis=0))
        acc[0] = m_new
        acc[1] = acc[1] * jnp.exp(m_old - m_new) + jnp.sum(jnp.exp(t3 - m_new), axis=0)
        row = lax.broadcasted_iota(jnp.int32, (n, 128), 0)
        hit = row == (tgt - base - lane_group * stride)
        acc[2] += jnp.sum(jnp.where(hit, t, 0.0).reshape(n // 8, 8, 128), axis=0)
        return t

    def put(t, n, base, stride):
        tt = t.T
        for g in range(G):
            logits_ref[:, pl.ds(pl.multiple_of(base + g * stride, 128), n)] = tt[g * tokens:(g + 1) * tokens, :]

    def finish_tail():
        b_tail().wait_recv()
        x_tail().wait_recv()
        x2_tail().wait_recv()
        t = update(tail_rows, rt, nf * rows, rt, rx2[...])
        tt = jnp.concatenate([t, jnp.zeros((128 - rt, 128), F32)], axis=0).T
        parts = [tt[g * tokens:(g + 1) * tokens, :] for g in range(G)]
        lane = lax.broadcasted_iota(jnp.int32, (tokens, 128), 1)
        for i in range((G * rt + 127) // 128):
            tile = jnp.zeros((tokens, 128), F32)
            for g in range(G):
                off = g * rt - i * 128
                if off <= -rt or off >= 128:
                    continue
                moved = pltpu.roll(parts[g], off % 128, 1) if off % 128 else parts[g]
                tile = jnp.where((lane >= off) & (lane < off + rt), moved, tile)
            logits_ref[:, nf * rows + i * 128:nf * rows + (i + 1) * 128] = tile
        b_tail().wait_send()
        x_tail().wait_send()
        x2_tail().wait_send()

    tail_copy(0).wait()
    ps[tail_rows, :] = packed_dot([tail.at[0]], rt)
    tail_copy(1).wait()
    po[tail_rows, :] = packed_dot([tail.at[1]], rt)
    pl.semaphore_wait(barrier, 3)
    x_tail().start()
    x2_tail().start()

    @pl.loop(0, nf + LATE - 1)
    def _(j):
        @pl.when(j < nf)
        def _():
            r_dot(j, 0, ps)

            @pl.when(j >= 2)
            def _():
                a_copy(j - 2).wait_send()

            a_copy(j).start()

        @pl.when(jnp.logical_and(j > 0, j <= nf))
        def _():
            add_sibling(j - 1)

        @pl.when(j == 1)
        def _():
            x_copy(j - 1).start()

        @pl.when(j < nf)
        def _():
            r_dot(j, 1, po)

        @pl.when(jnp.logical_and(j > 1, j < nf))
        def _():
            x_copy(j - 1).start()

        @pl.when(j < NL)
        def _():
            l_copy(j, 0).start()
            l_copy(j, 1).start()

        @pl.when(jnp.logical_and(j > LAG, j <= nf + LAG))
        def _():
            k = j - LAG - 1

            @pl.when(k >= 2)
            def _():
                b_copy(k - 2).wait_send()

            b_copy(k).start()

        @pl.when(jnp.logical_and(j >= LAG, j < nf + LAG))
        def _():
            l_dot(j - LAG)

        @pl.when(j == nf)
        def _():
            for p in range(2):
                x_piece(p).start()

        @pl.when(j == 4)
        def _():
            tail_copy(2).wait()
            tail_copy(3).wait()
            both = packed_dot([tail.at[2], tail.at[3]], rt)
            ls[tail_rows, :] = both[:rt]
            lo[tail_rows, :] = both[rt:]

        @pl.when(j == 5)
        def _():
            b_tail().start()

        @pl.when(j == 8)
        def _():
            finish_tail()

        @pl.when(j >= LATE)
        def _():
            k = j - LATE
            b_copy(k).wait_recv()
            x_copy(k).wait_recv()
            put(update(chunk(k), R, k * rows, R), R, k * rows, R)

            @pl.when(k > 0)
            def _():
                x_copy(k - 1).wait_send()

    for k in (last - 1, last):
        a_copy(k).wait_send()
        b_copy(k).wait_send()
    x_copy(last - 1).wait_send()
    b_copy(last).wait_recv()
    for p in range(2):
        x_piece(p).wait_recv()
        t = update(pl.ds(last * R + p * piece, piece), piece, last * rows + p * piece, R)
        put(t, piece, last * rows + p * piece, R)

    m = jnp.max(acc[0], axis=0, keepdims=True)
    norm = jnp.sum(acc[1] * jnp.exp(acc[0] - m), axis=0, keepdims=True)
    hit = jnp.sum(acc[2], axis=0, keepdims=True)
    st[me] = jnp.concatenate([m, norm, hit, jnp.zeros((5, 128), F32)], axis=0)
    for p in range(2):
        x_piece(p).wait_send()
    stat_copies = []
    for i, peer in enumerate((xpeer, diag, sib)):
        copy = pltpu.make_async_remote_copy(src_ref=st.at[me], dst_ref=st.at[me], send_sem=ss_sem.at[i],
                                            recv_sem=sr_sem.at[i], device_id={'tp': peer}, device_id_type=MESH)
        copy.start()
        stat_copies.append(copy)
    pick = lax.broadcasted_iota(jnp.int32, (tokens, 128), 0) == lax.broadcasted_iota(jnp.int32, (tokens, 128), 1)

    def column(row):
        return jnp.sum(jnp.where(pick, row, 0.0), axis=1, keepdims=True)

    own = functools.reduce(jnp.maximum, [pltpu.roll(m, shift, 1) for shift in range(tokens, G * tokens, tokens)], m)
    own_col = column(own)

    @pl.loop(0, nf)
    def _(k):
        sl = pl.ds(pl.multiple_of(k * rows, 128), rows)
        logits_ref[:, sl] = jnp.exp(logits_ref[:, sl] - own_col)

    sl = pl.ds(nf * rows, logits_ref.shape[1] - nf * rows)
    logits_ref[:, sl] = jnp.exp(logits_ref[:, sl] - own_col)
    for copy in stat_copies:
        copy.wait_send()
    for copy in stat_copies:
        copy.wait_recv()
    ms, ns, hit = [], [], jnp.zeros((1, 128), F32)
    for i in range(4):
        hit = hit + st[i, 2:3, :]
        for shift in range(0, G * tokens, tokens):
            ms.append(pltpu.roll(st[i, 0:1, :], shift, 1) if shift else st[i, 0:1, :])
            ns.append(pltpu.roll(st[i, 1:2, :], shift, 1) if shift else st[i, 1:2, :])
    hit = sum(pltpu.roll(hit, shift, 1) for shift in range(tokens, G * tokens, tokens)) + hit
    top = functools.reduce(jnp.maximum, ms)
    norm = sum(n * jnp.exp(m - top) for n, m in zip(ns, ms))
    log_norm = top + jnp.log(norm)
    stats_ref[...] = jnp.concatenate([log_norm, hit - log_norm, jnp.zeros((6, 128), F32)], axis=0)
    scale_ref[...] = jnp.broadcast_to(column(jnp.exp(own - log_norm)), (tokens, 128))


def probs_kernel(edges, exp_ref, stats_ref, scale_ref, ln_hbm, tl_hbm, probs_hbm, ln, tl, probs, sem, small_sem):
    tokens = ln.shape[1]
    ln[...] = stats_ref[0:1, :tokens]
    tl[...] = stats_ref[1:2, :tokens]
    copies = [pltpu.make_async_copy(ln, ln_hbm, small_sem.at[0]), pltpu.make_async_copy(tl, tl_hbm, small_sem.at[1])]
    scale = scale_ref[:, 0:1]
    for i, (start, stop) in enumerate(zip(edges, edges[1:])):
        sl = pl.ds(start, stop - start)
        probs[:, sl] = (exp_ref[:, sl] * scale).astype(BF16)
        if i == 0:
            for copy in copies:
                copy.start()
        pltpu.make_async_copy(probs.at[:, sl], probs_hbm.at[:, sl], sem.at[0]).start()
    copies.append(pltpu.make_async_copy(probs, probs_hbm, sem.at[0]))
    for copy in copies:
        copy.wait()


def solution(mesh):
    def local_scores(hidden, final_gain, table, targets, temperature):
        tokens, hidden_size = hidden.shape
        vocab, width = table.shape
        vq = vocab // 4
        nf = vq // (G * R)
        rt = (vq - nf * G * R) // G
        packed = vq // G
        lanes = (vq + 127) // 128 * 128
        dims = (tokens, hidden_size, width, vq, nf, rt)
        vmem = pl.BlockSpec(memory_space=pltpu.VMEM)
        hbm = pl.BlockSpec(memory_space=pltpu.HBM)
        exps, stats, scale = pl.pallas_call(
            functools.partial(scores_kernel, dims),
            out_shape=(pltpu.VMEM((tokens, lanes), F32), pltpu.VMEM((8, 128), F32), pltpu.VMEM((tokens, 128), F32)),
            in_specs=[pl.BlockSpec(memory_space=pltpu.SMEM), hbm, hbm, hbm, hbm],
            out_specs=(vmem, vmem, vmem),
            scratch_shapes=[
                pltpu.VMEM((1, tokens), jnp.int32),
                pltpu.VMEM((tokens, hidden_size), BF16),
                pltpu.VMEM((hidden_size // 128, 128), BF16),
                pltpu.VMEM((hidden_size // 128, 128), F32),
                pltpu.VMEM((G * width, 128), BF16),
                pltpu.VMEM((NR, 2, G * R, width), BF16),
                pltpu.VMEM((NL, 2, G * R, width), BF16),
                pltpu.VMEM((4, G * rt, width), BF16),
            ] + [pltpu.VMEM((packed, 128), F32)] * 7 + [
                pltpu.VMEM((rt, 128), F32),
                pltpu.VMEM((3, 8, 128), F32),
                pltpu.VMEM((4, 8, 128), F32),
                pltpu.SemaphoreType.DMA((3,)),
                pltpu.SemaphoreType.DMA((NR, 2)),
                pltpu.SemaphoreType.DMA((NL, 2)),
            ] + [pltpu.SemaphoreType.DMA((n,)) for n in (2, NA, 2, NB, NS, NX, 8)] + [
                pltpu.SemaphoreType.DMA((3,)),
                pltpu.SemaphoreType.DMA((3,)),
            ],
            compiler_params=pltpu.CompilerParams(collective_id=0, has_side_effects=True,
                                                 vmem_limit_bytes=54 * 2 ** 20),
        )(temperature.reshape(1, 1), targets.reshape(1, tokens), hidden, final_gain.reshape(hidden_size // 128, 128), table)
        edges = [0, 1024, 3072, 7168] + list(range(13312, vq - 4096, 6144)) + [vq]
        log_norm, target_logprob, probs = pl.pallas_call(
            functools.partial(probs_kernel, edges),
            out_shape=(jax.ShapeDtypeStruct((1, tokens), F32),
                       jax.ShapeDtypeStruct((1, tokens), F32),
                       jax.ShapeDtypeStruct((tokens, vq), BF16)),
            in_specs=[vmem, vmem, vmem],
            out_specs=(hbm, hbm, hbm),
            scratch_shapes=[pltpu.VMEM((1, tokens), F32), pltpu.VMEM((1, tokens), F32),
                            pltpu.VMEM((tokens, vq), BF16),
                            pltpu.SemaphoreType.DMA((1,)), pltpu.SemaphoreType.DMA((2,))],
            compiler_params=pltpu.CompilerParams(vmem_limit_bytes=8 * 2 ** 20),
        )(exps, stats, scale)
        return log_norm.reshape(tokens), target_logprob.reshape(tokens), probs

    return jax.shard_map(local_scores, mesh=mesh,
                         in_specs=(P('dp', None), P(None), P(None, 'tp'), P('dp'), P()),
                         out_specs=(P('dp'), P('dp'), P('dp', 'tp')),
                         check_vma=False)
```

```python
import functools

import jax
import jax.numpy as jnp
from jax import lax
from jax.experimental import pallas as pl
from jax.experimental.pallas import tpu as pltpu
from jax.sharding import PartitionSpec as P

NORM_EPS = 1e-6
MESH = pl.DeviceIdType.MESH
F32 = jnp.float32
BF16 = jnp.bfloat16
G = 4
R = 256
NR = 2
NL = 2
LAG = 2
LATE = 4
NA, NB, NS, NX = 5, 5, 5, 2 * LATE


def scores_kernel(dims, temp_ref, tgt_hbm, hid_hbm, gain_hbm, table, logits_ref, stats_ref, scale_ref,
                  tgt_ref, hid, gain, gain32, w, ring_r, ring_l, tail, ps, po, ls, lo, ra, rb, rx, rx2, acc, st,
                  in_sem, r_sem, l_sem, as_sem, ar_sem, bs_sem, br_sem, xs_sem, xr_sem, one_sem):
    tokens, hidden_size, width, vq, nf, rt = dims
    me = lax.axis_index('tp')
    x = me // 2
    c = me % 2
    sib = 2 * x + (1 - c)
    xpeer = 2 * (1 - x) + c
    diag = 2 * (1 - x) + (1 - c)
    rows = G * R
    trows = G * rt
    last = nf - 1

    def quarter(chip, half):
        return (2 * chip + ((1 - c) if half == 0 else c)) * vq

    def r_copy(k, half):
        start = pl.multiple_of(quarter(1 - x, half) + k * rows, 64)
        return pltpu.make_async_copy(table.at[pl.ds(start, rows)], ring_r.at[k % NR, half], r_sem.at[k % NR, half])

    def l_copy(k, half):
        start = pl.multiple_of(quarter(x, half) + k * rows, 64)
        return pltpu.make_async_copy(table.at[pl.ds(start, rows)], ring_l.at[k % NL, half], l_sem.at[k % NL, half])

    def tail_copy(i):
        start = pl.multiple_of(quarter((1 - x) if i < 2 else x, i % 2) + nf * rows, 64)
        return pltpu.make_async_copy(table.at[pl.ds(start, trows)], tail.at[i], (l_sem.at[0, i] if i < 2 else in_sem.at[i - 2]))

    def chunk(k):
        return pl.ds(pl.multiple_of(k * R, R), R)

    tail_rows = pl.ds(nf * R, rt)

    def remote(src, dst, send, recv, dev):
        return pltpu.make_async_remote_copy(src_ref=src, dst_ref=dst, send_sem=send, recv_sem=recv,
                                            device_id={'tp': dev}, device_id_type=MESH)

    def a_copy(k):
        sl = chunk(k)
        return remote(ps.at[sl], ra.at[sl], as_sem.at[k % 2], ar_sem.at[k % NA], sib)

    def b_copy(k):
        sl = chunk(k)
        return remote(ls.at[sl], rb.at[sl], bs_sem.at[k % 2], br_sem.at[k % NB], sib)

    def x_copy(k):
        sl = chunk(k)
        return remote(po.at[sl], rx.at[sl], xs_sem.at[k % NS], xr_sem.at[k % NX], xpeer)

    def b_tail():
        return remote(ls.at[tail_rows], rb.at[tail_rows], one_sem.at[0], one_sem.at[1], sib)

    def x_tail():
        return remote(po.at[tail_rows], rx.at[tail_rows], one_sem.at[2], one_sem.at[3], xpeer)

    def x2_tail():
        return remote(ps.at[tail_rows], rx2, one_sem.at[4], one_sem.at[5], diag)

    piece = R // 2

    def x_piece(p):
        sl = pl.ds(last * R + p * piece, piece)
        send, recv = (one_sem.at[6], one_sem.at[7]) if p else (xs_sem.at[last % NS], xr_sem.at[last % NX])
        return remote(po.at[sl], rx.at[sl], send, recv, xpeer)

    hid_copy = pltpu.make_async_copy(hid_hbm, hid, in_sem.at[0])
    gain_copy = pltpu.make_async_copy(gain_hbm, gain, in_sem.at[1])
    tgt_copy = pltpu.make_async_copy(tgt_hbm, tgt_ref, in_sem.at[2])
    hid_copy.start()
    gain_copy.start()
    tgt_copy.start()
    tail_copy(0).start()
    tail_copy(1).start()

    barrier = pltpu.get_barrier_semaphore()
    for peer in (sib, xpeer, diag):
        pl.semaphore_signal(barrier, inc=1, device_id={'tp': peer}, device_id_type=MESH)

    hid_copy.wait()
    gain_copy.wait()
    for k in range(NR):
        r_copy(k, 0).start()
        r_copy(k, 1).start()
    tail_copy(2).start()
    tail_copy(3).start()

    hf = hid[...].astype(F32)
    inv = lax.rsqrt(jnp.mean(hf * hf, axis=-1, keepdims=True) + NORM_EPS)
    cols = pl.ds(pl.multiple_of(me * width, 128), width)
    gain32[...] = gain[...].astype(F32)
    scaled = hid[:, cols].astype(F32) * inv
    u = jnp.concatenate([scaled[:, j * 128:(j + 1) * 128] * gain32[pl.ds(me * (width // 128) + j, 1), :]
                         for j in range(width // 128)], axis=1).astype(BF16).astype(F32)
    u_t = jnp.concatenate([u] * G, axis=0).T
    group = lax.broadcasted_iota(jnp.int32, (width, 128), 1) // tokens
    for g in range(G):
        w[g * width:(g + 1) * width, :] = jnp.where(group == g, u_t, 0.0).astype(BF16)
    acc[0] = jnp.full((8, 128), -jnp.inf, F32)
    acc[1] = jnp.zeros((8, 128), F32)
    acc[2] = jnp.zeros((8, 128), F32)
    temp = temp_ref[0, 0]
    lane_group = lax.broadcasted_iota(jnp.int32, (1, 128), 1) // tokens
    tgt_copy.wait()
    tgt = jnp.concatenate([tgt_ref[...]] * G, axis=1) - me * vq

    def packed_dot(views, n):
        total = None
        for g in range(G):
            parts = [view[g * n:(g + 1) * n, :] for view in views]
            lhs = parts[0] if len(parts) == 1 else jnp.concatenate(parts, axis=0)
            part = jnp.dot(lhs, w[g * width:(g + 1) * width, :], preferred_element_type=F32)
            total = part if total is None else total + part
        return total

    def r_dot(k, half, dst):
        r_copy(k, half).wait()
        dst[chunk(k), :] = packed_dot([ring_r.at[k % NR, half]], R)

        @pl.when(k + NR < nf)
        def _():
            r_copy(k + NR, half).start()

    def l_dot(k):
        l_copy(k, 0).wait()
        l_copy(k, 1).wait()
        both = packed_dot([ring_l.at[k % NL, 0], ring_l.at[k % NL, 1]], R)
        ls[chunk(k), :] = both[:R]
        lo[chunk(k), :] = both[R:]

        @pl.when(k + NL < nf)
        def _():
            l_copy(k + NL, 0).start()
            l_copy(k + NL, 1).start()

    def add_sibling(k):
        sl = chunk(k)
        a_copy(k).wait_recv()
        po[sl, :] = po[sl, :] + ra[sl, :]

    def update(sl, n, base, stride, crossed=None):
        z = lo[sl, :] + rb[sl, :] + rx[sl, :]
        t = (z if crossed is None else z + crossed) / temp
        t3 = t.reshape(n // 8, 8, 128)
        m_old = acc[0]
        m_new = jnp.maximum(m_old, jnp.max(t3, axis=0))
        acc[0] = m_new
        acc[1] = acc[1] * jnp.exp(m_old - m_new) + jnp.sum(jnp.exp(t3 - m_new), axis=0)
        row = lax.broadcasted_iota(jnp.int32, (n, 128), 0)
        hit = row == (tgt - base - lane_group * stride)
        acc[2] += jnp.sum(jnp.where(hit, t, 0.0).reshape(n // 8, 8, 128), axis=0)
        return t

    def put(t, n, base, stride):
        tt = t.T
        for g in range(G):
            logits_ref[:, pl.ds(pl.multiple_of(base + g * stride, 128), n)] = tt[g * tokens:(g + 1) * tokens, :]

    def finish_tail():
        b_tail().wait_recv()
        x_tail().wait_recv()
        x2_tail().wait_recv()
        t = update(tail_rows, rt, nf * rows, rt, rx2[...])
        tt = jnp.concatenate([t, jnp.zeros((128 - rt, 128), F32)], axis=0).T
        parts = [tt[g * tokens:(g + 1) * tokens, :] for g in range(G)]
        lane = lax.broadcasted_iota(jnp.int32, (tokens, 128), 1)
        for i in range((G * rt + 127) // 128):
            tile = jnp.zeros((tokens, 128), F32)
            for g in range(G):
                off = g * rt - i * 128
                if off <= -rt or off >= 128:
                    continue
                moved = pltpu.roll(parts[g], off % 128, 1) if off % 128 else parts[g]
                tile = jnp.where((lane >= off) & (lane < off + rt), moved, tile)
            logits_ref[:, nf * rows + i * 128:nf * rows + (i + 1) * 128] = tile
        b_tail().wait_send()
        x_tail().wait_send()
        x2_tail().wait_send()

    tail_copy(0).wait()
    ps[tail_rows, :] = packed_dot([tail.at[0]], rt)
    tail_copy(1).wait()
    po[tail_rows, :] = packed_dot([tail.at[1]], rt)
    pl.semaphore_wait(barrier, 3)
    x_tail().start()
    x2_tail().start()

    @pl.loop(0, nf + LATE - 1)
    def _(j):
        @pl.when(j < nf)
        def _():
            r_dot(j, 0, ps)

            @pl.when(j >= 2)
            def _():
                a_copy(j - 2).wait_send()

            a_copy(j).start()

        @pl.when(jnp.logical_and(j > 0, j <= nf))
        def _():
            add_sibling(j - 1)

        @pl.when(j == 1)
        def _():
            x_copy(j - 1).start()

        @pl.when(j < nf)
        def _():
            r_dot(j, 1, po)

        @pl.when(jnp.logical_and(j > 1, j < nf))
        def _():
            x_copy(j - 1).start()

        @pl.when(j < NL)
        def _():
            l_copy(j, 0).start()
            l_copy(j, 1).start()

        @pl.when(jnp.logical_and(j > LAG, j <= nf + LAG))
        def _():
            k = j - LAG - 1

            @pl.when(k >= 2)
            def _():
                b_copy(k - 2).wait_send()

            b_copy(k).start()

        @pl.when(jnp.logical_and(j >= LAG, j < nf + LAG))
        def _():
            l_dot(j - LAG)

        @pl.when(j == nf)
        def _():
            for p in range(2):
                x_piece(p).start()

        @pl.when(j == 4)
        def _():
            tail_copy(2).wait()
            tail_copy(3).wait()
            both = packed_dot([tail.at[2], tail.at[3]], rt)
            ls[tail_rows, :] = both[:rt]
            lo[tail_rows, :] = both[rt:]

        @pl.when(j == 5)
        def _():
            b_tail().start()

        @pl.when(j == 8)
        def _():
            finish_tail()

        @pl.when(j >= LATE)
        def _():
            k = j - LATE
            b_copy(k).wait_recv()
            x_copy(k).wait_recv()
            put(update(chunk(k), R, k * rows, R), R, k * rows, R)

            @pl.when(k > 0)
            def _():
                x_copy(k - 1).wait_send()

    for k in (last - 1, last):
        a_copy(k).wait_send()
        b_copy(k).wait_send()
    x_copy(last - 1).wait_send()
    b_copy(last).wait_recv()
    for p in range(2):
        x_piece(p).wait_recv()
        t = update(pl.ds(last * R + p * piece, piece), piece, last * rows + p * piece, R)
        put(t, piece, last * rows + p * piece, R)

    m = jnp.max(acc[0], axis=0, keepdims=True)
    norm = jnp.sum(acc[1] * jnp.exp(acc[0] - m), axis=0, keepdims=True)
    hit = jnp.sum(acc[2], axis=0, keepdims=True)
    st[me] = jnp.concatenate([m, norm, hit, jnp.zeros((5, 128), F32)], axis=0)
    for p in range(2):
        x_piece(p).wait_send()
    stat_copies = []
    for peer, send, recv in ((xpeer, as_sem.at[0], one_sem.at[3]), (diag, as_sem.at[1], one_sem.at[5]),
                             (sib, bs_sem.at[0], one_sem.at[1])):
        copy = pltpu.make_async_remote_copy(src_ref=st.at[me], dst_ref=st.at[me], send_sem=send,
                                            recv_sem=recv, device_id={'tp': peer}, device_id_type=MESH)
        copy.start()
        stat_copies.append(copy)
    pick = lax.broadcasted_iota(jnp.int32, (tokens, 128), 0) == lax.broadcasted_iota(jnp.int32, (tokens, 128), 1)

    def column(row):
        return jnp.sum(jnp.where(pick, row, 0.0), axis=1, keepdims=True)

    own = functools.reduce(jnp.maximum, [pltpu.roll(m, shift, 1) for shift in range(tokens, G * tokens, tokens)], m)
    own_col = column(own)

    @pl.loop(0, nf)
    def _(k):
        sl = pl.ds(pl.multiple_of(k * rows, 128), rows)
        logits_ref[:, sl] = jnp.exp(logits_ref[:, sl] - own_col)

    sl = pl.ds(nf * rows, logits_ref.shape[1] - nf * rows)
    logits_ref[:, sl] = jnp.exp(logits_ref[:, sl] - own_col)
    for copy in stat_copies:
        copy.wait_send()
    for copy in stat_copies:
        copy.wait_recv()
    ms, ns, hit = [], [], jnp.zeros((1, 128), F32)
    for i in range(4):
        hit = hit + st[i, 2:3, :]
        for shift in range(0, G * tokens, tokens):
            ms.append(pltpu.roll(st[i, 0:1, :], shift, 1) if shift else st[i, 0:1, :])
            ns.append(pltpu.roll(st[i, 1:2, :], shift, 1) if shift else st[i, 1:2, :])
    hit = sum(pltpu.roll(hit, shift, 1) for shift in range(tokens, G * tokens, tokens)) + hit
    top = functools.reduce(jnp.maximum, ms)
    norm = sum(n * jnp.exp(m - top) for n, m in zip(ns, ms))
    log_norm = top + jnp.log(norm)
    stats_ref[...] = jnp.concatenate([log_norm, hit - log_norm, jnp.zeros((6, 128), F32)], axis=0)
    scale_ref[...] = jnp.broadcast_to(column(jnp.exp(own - log_norm)), (tokens, 128))


def probs_kernel(edges, exp_ref, stats_ref, scale_ref, ln_hbm, tl_hbm, probs_hbm, ln, tl, probs, sem, small_sem):
    tokens = ln.shape[1]
    ln[...] = stats_ref[0:1, :tokens]
    tl[...] = stats_ref[1:2, :tokens]
    copies = [pltpu.make_async_copy(ln, ln_hbm, small_sem.at[0]), pltpu.make_async_copy(tl, tl_hbm, small_sem.at[1])]
    scale = scale_ref[:, 0:1]
    for i, (start, stop) in enumerate(zip(edges, edges[1:])):
        sl = pl.ds(start, stop - start)
        probs[:, sl] = (exp_ref[:, sl] * scale).astype(BF16)
        if i == 0:
            for copy in copies:
                copy.start()
        pltpu.make_async_copy(probs.at[:, sl], probs_hbm.at[:, sl], sem.at[0]).start()
    copies.append(pltpu.make_async_copy(probs, probs_hbm, sem.at[0]))
    for copy in copies:
        copy.wait()


def solution(mesh):
    def local_scores(hidden, final_gain, table, targets, temperature):
        tokens, hidden_size = hidden.shape
        vocab, width = table.shape
        vq = vocab // 4
        nf = vq // (G * R)
        rt = (vq - nf * G * R) // G
        packed = vq // G
        lanes = (vq + 127) // 128 * 128
        dims = (tokens, hidden_size, width, vq, nf, rt)
        vmem = pl.BlockSpec(memory_space=pltpu.VMEM)
        hbm = pl.BlockSpec(memory_space=pltpu.HBM)
        exps, stats, scale = pl.pallas_call(
            functools.partial(scores_kernel, dims),
            out_shape=(pltpu.VMEM((tokens, lanes), F32), pltpu.VMEM((8, 128), F32), pltpu.VMEM((tokens, 128), F32)),
            in_specs=[pl.BlockSpec(memory_space=pltpu.SMEM), hbm, hbm, hbm, hbm],
            out_specs=(vmem, vmem, vmem),
            scratch_shapes=[
                pltpu.VMEM((1, tokens), jnp.int32),
                pltpu.VMEM((tokens, hidden_size), BF16),
                pltpu.VMEM((hidden_size // 128, 128), BF16),
                pltpu.VMEM((hidden_size // 128, 128), F32),
                pltpu.VMEM((G * width, 128), BF16),
                pltpu.VMEM((NR, 2, G * R, width), BF16),
                pltpu.VMEM((NL, 2, G * R, width), BF16),
                pltpu.VMEM((4, G * rt, width), BF16),
            ] + [pltpu.VMEM((packed, 128), F32)] * 7 + [
                pltpu.VMEM((rt, 128), F32),
                pltpu.VMEM((3, 8, 128), F32),
                pltpu.VMEM((4, 8, 128), F32),
                pltpu.SemaphoreType.DMA((3,)),
                pltpu.SemaphoreType.DMA((NR, 2)),
                pltpu.SemaphoreType.DMA((NL, 2)),
            ] + [pltpu.SemaphoreType.DMA((n,)) for n in (2, NA, 2, NB, NS, NX, 8)],
            compiler_params=pltpu.CompilerParams(collective_id=0, has_side_effects=True,
                                                 vmem_limit_bytes=54 * 2 ** 20),
        )(temperature.reshape(1, 1), targets.reshape(1, tokens), hidden, final_gain.reshape(hidden_size // 128, 128), table)
        edges = [0, 1024, 3072, 7168] + list(range(13312, vq - 4096, 6144)) + [vq]
        log_norm, target_logprob, probs = pl.pallas_call(
            functools.partial(probs_kernel, edges),
            out_shape=(jax.ShapeDtypeStruct((1, tokens), F32),
                       jax.ShapeDtypeStruct((1, tokens), F32),
                       jax.ShapeDtypeStruct((tokens, vq), BF16)),
            in_specs=[vmem, vmem, vmem],
            out_specs=(hbm, hbm, hbm),
            scratch_shapes=[pltpu.VMEM((1, tokens), F32), pltpu.VMEM((1, tokens), F32),
                            pltpu.VMEM((tokens, vq), BF16),
                            pltpu.SemaphoreType.DMA((1,)), pltpu.SemaphoreType.DMA((2,))],
            compiler_params=pltpu.CompilerParams(vmem_limit_bytes=8 * 2 ** 20),
        )(exps, stats, scale)
        return log_norm.reshape(tokens), target_logprob.reshape(tokens), probs

    return jax.shard_map(local_scores, mesh=mesh,
                         in_specs=(P('dp', None), P(None), P(None, 'tp'), P('dp'), P()),
                         out_specs=(P('dp'), P('dp'), P('dp', 'tp')),
                         check_vma=False)
```

```python
import functools

import jax
import jax.numpy as jnp
from jax import lax
from jax.experimental import pallas as pl
from jax.experimental.pallas import tpu as pltpu
from jax.sharding import PartitionSpec as P

NORM_EPS = 1e-6
MESH = pl.DeviceIdType.MESH
F32 = jnp.float32
BF16 = jnp.bfloat16
G = 4
R = 256
NR = 2
NL = 2
LAG = 2
LATE = 4
NA, NB, NS, NX = 4, 4, 5, 2 * LATE


def scores_kernel(dims, temp_ref, tgt_hbm, hid_hbm, gain_hbm, table, logits_ref, stats_ref, scale_ref,
                  tgt_ref, hid, gain, gain32, w, ring_r, ring_l, tail, ps, po, ls, lo, ra, rb, rx, rx2, acc, st,
                  in_sem, r_sem, l_sem, as_sem, ar_sem, bs_sem, br_sem, xs_sem, xr_sem, one_sem):
    tokens, hidden_size, width, vq, nf, rt = dims
    me = lax.axis_index('tp')
    x = me // 2
    c = me % 2
    sib = 2 * x + (1 - c)
    xpeer = 2 * (1 - x) + c
    diag = 2 * (1 - x) + (1 - c)
    rows = G * R
    trows = G * rt
    last = nf - 1

    def quarter(chip, half):
        return (2 * chip + ((1 - c) if half == 0 else c)) * vq

    def r_copy(k, half):
        start = pl.multiple_of(quarter(1 - x, half) + k * rows, 64)
        return pltpu.make_async_copy(table.at[pl.ds(start, rows)], ring_r.at[k % NR, half], r_sem.at[k % NR, half])

    def l_copy(k, half):
        start = pl.multiple_of(quarter(x, half) + k * rows, 64)
        return pltpu.make_async_copy(table.at[pl.ds(start, rows)], ring_l.at[k % NL, half], l_sem.at[k % NL, half])

    def tail_copy(i):
        start = pl.multiple_of(quarter((1 - x) if i < 2 else x, i % 2) + nf * rows, 64)
        return pltpu.make_async_copy(table.at[pl.ds(start, trows)], tail.at[i], (l_sem.at[0, i] if i < 2 else in_sem.at[i - 2]))

    def chunk(k):
        return pl.ds(pl.multiple_of(k * R, R), R)

    tail_rows = pl.ds(nf * R, rt)

    def remote(src, dst, send, recv, dev):
        return pltpu.make_async_remote_copy(src_ref=src, dst_ref=dst, send_sem=send, recv_sem=recv,
                                            device_id={'tp': dev}, device_id_type=MESH)

    def a_copy(k):
        sl = chunk(k)
        return remote(ps.at[sl], ra.at[sl], as_sem.at[k % 2], ar_sem.at[k % NA], sib)

    def b_copy(k):
        sl = chunk(k)
        return remote(ls.at[sl], rb.at[sl], bs_sem.at[k % 2], br_sem.at[k % NB], sib)

    def x_copy(k):
        sl = chunk(k)
        return remote(po.at[sl], rx.at[sl], xs_sem.at[k % NS], xr_sem.at[k % NX], xpeer)

    def b_tail():
        return remote(ls.at[tail_rows], rb.at[tail_rows], one_sem.at[0], one_sem.at[1], sib)

    def x_tail():
        return remote(po.at[tail_rows], rx.at[tail_rows], one_sem.at[2], one_sem.at[3], xpeer)

    def x2_tail():
        return remote(ps.at[tail_rows], rx2, one_sem.at[4], one_sem.at[5], diag)

    piece = R // 2

    def x_piece(p):
        sl = pl.ds(last * R + p * piece, piece)
        send, recv = (one_sem.at[6], one_sem.at[7]) if p else (xs_sem.at[last % NS], xr_sem.at[last % NX])
        return remote(po.at[sl], rx.at[sl], send, recv, xpeer)

    hid_copy = pltpu.make_async_copy(hid_hbm, hid, in_sem.at[0])
    gain_copy = pltpu.make_async_copy(gain_hbm, gain, in_sem.at[1])
    tgt_copy = pltpu.make_async_copy(tgt_hbm, tgt_ref, in_sem.at[2])
    hid_copy.start()
    gain_copy.start()
    tgt_copy.start()
    tail_copy(0).start()
    tail_copy(1).start()

    barrier = pltpu.get_barrier_semaphore()
    for peer in (sib, xpeer, diag):
        pl.semaphore_signal(barrier, inc=1, device_id={'tp': peer}, device_id_type=MESH)

    hid_copy.wait()
    gain_copy.wait()
    for k in range(NR):
        r_copy(k, 0).start()
        r_copy(k, 1).start()
    tail_copy(2).start()
    tail_copy(3).start()

    hf = hid[...].astype(F32)
    inv = lax.rsqrt(jnp.mean(hf * hf, axis=-1, keepdims=True) + NORM_EPS)
    cols = pl.ds(pl.multiple_of(me * width, 128), width)
    gain32[...] = gain[...].astype(F32)
    scaled = hid[:, cols].astype(F32) * inv
    u = jnp.concatenate([scaled[:, j * 128:(j + 1) * 128] * gain32[pl.ds(me * (width // 128) + j, 1), :]
                         for j in range(width // 128)], axis=1).astype(BF16).astype(F32)
    u_t = jnp.concatenate([u] * G, axis=0).T
    group = lax.broadcasted_iota(jnp.int32, (width, 128), 1) // tokens
    for g in range(G):
        w[g * width:(g + 1) * width, :] = jnp.where(group == g, u_t, 0.0).astype(BF16)
    acc[0] = jnp.full((8, 128), -jnp.inf, F32)
    acc[1] = jnp.zeros((8, 128), F32)
    acc[2] = jnp.zeros((8, 128), F32)
    temp = temp_ref[0, 0]
    lane_group = lax.broadcasted_iota(jnp.int32, (1, 128), 1) // tokens
    tgt_copy.wait()
    tgt = jnp.concatenate([tgt_ref[...]] * G, axis=1) - me * vq

    def packed_dot(views, n):
        total = None
        for g in range(G):
            parts = [view[g * n:(g + 1) * n, :] for view in views]
            lhs = parts[0] if len(parts) == 1 else jnp.concatenate(parts, axis=0)
            part = jnp.dot(lhs, w[g * width:(g + 1) * width, :], preferred_element_type=F32)
            total = part if total is None else total + part
        return total

    def r_dot(k, half, dst):
        r_copy(k, half).wait()
        dst[chunk(k), :] = packed_dot([ring_r.at[k % NR, half]], R)

        @pl.when(k + NR < nf)
        def _():
            r_copy(k + NR, half).start()

    def l_dot(k):
        l_copy(k, 0).wait()
        l_copy(k, 1).wait()
        both = packed_dot([ring_l.at[k % NL, 0], ring_l.at[k % NL, 1]], R)
        ls[chunk(k), :] = both[:R]
        lo[chunk(k), :] = both[R:]

        @pl.when(k + NL < nf)
        def _():
            l_copy(k + NL, 0).start()
            l_copy(k + NL, 1).start()

    def add_sibling(k):
        sl = chunk(k)
        a_copy(k).wait_recv()
        po[sl, :] = po[sl, :] + ra[sl, :]

    def update(sl, n, base, stride, crossed=None):
        z = lo[sl, :] + rb[sl, :] + rx[sl, :]
        t = (z if crossed is None else z + crossed) / temp
        t3 = t.reshape(n // 8, 8, 128)
        m_old = acc[0]
        m_new = jnp.maximum(m_old, jnp.max(t3, axis=0))
        acc[0] = m_new
        acc[1] = acc[1] * jnp.exp(m_old - m_new) + jnp.sum(jnp.exp(t3 - m_new), axis=0)
        row = lax.broadcasted_iota(jnp.int32, (n, 128), 0)
        hit = row == (tgt - base - lane_group * stride)
        acc[2] += jnp.sum(jnp.where(hit, t, 0.0).reshape(n // 8, 8, 128), axis=0)
        return t

    def put(t, n, base, stride):
        tt = t.T
        for g in range(G):
            logits_ref[:, pl.ds(pl.multiple_of(base + g * stride, 128), n)] = tt[g * tokens:(g + 1) * tokens, :]

    def finish_tail():
        b_tail().wait_recv()
        x_tail().wait_recv()
        x2_tail().wait_recv()
        t = update(tail_rows, rt, nf * rows, rt, rx2[...])
        tt = jnp.concatenate([t, jnp.zeros((128 - rt, 128), F32)], axis=0).T
        parts = [tt[g * tokens:(g + 1) * tokens, :] for g in range(G)]
        lane = lax.broadcasted_iota(jnp.int32, (tokens, 128), 1)
        for i in range((G * rt + 127) // 128):
            tile = jnp.zeros((tokens, 128), F32)
            for g in range(G):
                off = g * rt - i * 128
                if off <= -rt or off >= 128:
                    continue
                moved = pltpu.roll(parts[g], off % 128, 1) if off % 128 else parts[g]
                tile = jnp.where((lane >= off) & (lane < off + rt), moved, tile)
            logits_ref[:, nf * rows + i * 128:nf * rows + (i + 1) * 128] = tile
        b_tail().wait_send()
        x_tail().wait_send()
        x2_tail().wait_send()

    tail_copy(0).wait()
    ps[tail_rows, :] = packed_dot([tail.at[0]], rt)
    tail_copy(1).wait()
    po[tail_rows, :] = packed_dot([tail.at[1]], rt)
    pl.semaphore_wait(barrier, 3)
    x_tail().start()
    x2_tail().start()

    @pl.loop(0, nf + LATE - 1)
    def _(j):
        @pl.when(j < nf)
        def _():
            r_dot(j, 0, ps)

            @pl.when(j >= 2)
            def _():
                a_copy(j - 2).wait_send()

            a_copy(j).start()

        @pl.when(jnp.logical_and(j > 0, j <= nf))
        def _():
            add_sibling(j - 1)

        @pl.when(j == 1)
        def _():
            x_copy(j - 1).start()

        @pl.when(j < nf)
        def _():
            r_dot(j, 1, po)

        @pl.when(jnp.logical_and(j > 1, j < nf))
        def _():
            x_copy(j - 1).start()

        @pl.when(j < NL)
        def _():
            l_copy(j, 0).start()
            l_copy(j, 1).start()

        @pl.when(jnp.logical_and(j > LAG, j <= nf + LAG))
        def _():
            k = j - LAG - 1

            @pl.when(k >= 2)
            def _():
                b_copy(k - 2).wait_send()

            b_copy(k).start()

        @pl.when(jnp.logical_and(j >= LAG, j < nf + LAG))
        def _():
            l_dot(j - LAG)

        @pl.when(j == nf)
        def _():
            for p in range(2):
                x_piece(p).start()

        @pl.when(j == 4)
        def _():
            tail_copy(2).wait()
            tail_copy(3).wait()
            both = packed_dot([tail.at[2], tail.at[3]], rt)
            ls[tail_rows, :] = both[:rt]
            lo[tail_rows, :] = both[rt:]

        @pl.when(j == 5)
        def _():
            b_tail().start()

        @pl.when(j == 8)
        def _():
            finish_tail()

        @pl.when(j >= LATE)
        def _():
            k = j - LATE
            b_copy(k).wait_recv()
            x_copy(k).wait_recv()
            put(update(chunk(k), R, k * rows, R), R, k * rows, R)

            @pl.when(k > 0)
            def _():
                x_copy(k - 1).wait_send()

    for k in (last - 1, last):
        a_copy(k).wait_send()
        b_copy(k).wait_send()
    x_copy(last - 1).wait_send()
    b_copy(last).wait_recv()
    for p in range(2):
        x_piece(p).wait_recv()
        t = update(pl.ds(last * R + p * piece, piece), piece, last * rows + p * piece, R)
        put(t, piece, last * rows + p * piece, R)

    m = jnp.max(acc[0], axis=0, keepdims=True)
    norm = jnp.sum(acc[1] * jnp.exp(acc[0] - m), axis=0, keepdims=True)
    hit = jnp.sum(acc[2], axis=0, keepdims=True)
    st[me] = jnp.concatenate([m, norm, hit, jnp.zeros((5, 128), F32)], axis=0)
    for p in range(2):
        x_piece(p).wait_send()
    stat_copies = []
    for peer, send, recv in ((xpeer, as_sem.at[0], one_sem.at[3]), (diag, as_sem.at[1], one_sem.at[5]),
                             (sib, bs_sem.at[0], one_sem.at[1])):
        copy = pltpu.make_async_remote_copy(src_ref=st.at[me], dst_ref=st.at[me], send_sem=send,
                                            recv_sem=recv, device_id={'tp': peer}, device_id_type=MESH)
        copy.start()
        stat_copies.append(copy)
    pick = lax.broadcasted_iota(jnp.int32, (tokens, 128), 0) == lax.broadcasted_iota(jnp.int32, (tokens, 128), 1)

    def column(row):
        return jnp.sum(jnp.where(pick, row, 0.0), axis=1, keepdims=True)

    own = functools.reduce(jnp.maximum, [pltpu.roll(m, shift, 1) for shift in range(tokens, G * tokens, tokens)], m)
    own_col = column(own)

    @pl.loop(0, nf)
    def _(k):
        sl = pl.ds(pl.multiple_of(k * rows, 128), rows)
        logits_ref[:, sl] = jnp.exp(logits_ref[:, sl] - own_col)

    sl = pl.ds(nf * rows, logits_ref.shape[1] - nf * rows)
    logits_ref[:, sl] = jnp.exp(logits_ref[:, sl] - own_col)
    for copy in stat_copies:
        copy.wait_send()
    for copy in stat_copies:
        copy.wait_recv()
    ms, ns, hit = [], [], jnp.zeros((1, 128), F32)
    for i in range(4):
        hit = hit + st[i, 2:3, :]
        for shift in range(0, G * tokens, tokens):
            ms.append(pltpu.roll(st[i, 0:1, :], shift, 1) if shift else st[i, 0:1, :])
            ns.append(pltpu.roll(st[i, 1:2, :], shift, 1) if shift else st[i, 1:2, :])
    hit = sum(pltpu.roll(hit, shift, 1) for shift in range(tokens, G * tokens, tokens)) + hit
    top = functools.reduce(jnp.maximum, ms)
    norm = sum(n * jnp.exp(m - top) for n, m in zip(ns, ms))
    log_norm = top + jnp.log(norm)
    stats_ref[...] = jnp.concatenate([log_norm, hit - log_norm, jnp.zeros((6, 128), F32)], axis=0)
    scale_ref[...] = jnp.broadcast_to(column(jnp.exp(own - log_norm)), (tokens, 128))


def probs_kernel(edges, exp_ref, stats_ref, scale_ref, ln_hbm, tl_hbm, probs_hbm, ln, tl, probs, sem, small_sem):
    tokens = ln.shape[1]
    ln[...] = stats_ref[0:1, :tokens]
    tl[...] = stats_ref[1:2, :tokens]
    copies = [pltpu.make_async_copy(ln, ln_hbm, small_sem.at[0]), pltpu.make_async_copy(tl, tl_hbm, small_sem.at[1])]
    scale = scale_ref[:, 0:1]
    for i, (start, stop) in enumerate(zip(edges, edges[1:])):
        sl = pl.ds(start, stop - start)
        probs[:, sl] = (exp_ref[:, sl] * scale).astype(BF16)
        if i == 0:
            for copy in copies:
                copy.start()
        pltpu.make_async_copy(probs.at[:, sl], probs_hbm.at[:, sl], sem.at[0]).start()
    copies.append(pltpu.make_async_copy(probs, probs_hbm, sem.at[0]))
    for copy in copies:
        copy.wait()


def solution(mesh):
    def local_scores(hidden, final_gain, table, targets, temperature):
        tokens, hidden_size = hidden.shape
        vocab, width = table.shape
        vq = vocab // 4
        nf = vq // (G * R)
        rt = (vq - nf * G * R) // G
        packed = vq // G
        lanes = (vq + 127) // 128 * 128
        dims = (tokens, hidden_size, width, vq, nf, rt)
        vmem = pl.BlockSpec(memory_space=pltpu.VMEM)
        hbm = pl.BlockSpec(memory_space=pltpu.HBM)
        exps, stats, scale = pl.pallas_call(
            functools.partial(scores_kernel, dims),
            out_shape=(pltpu.VMEM((tokens, lanes), F32), pltpu.VMEM((8, 128), F32), pltpu.VMEM((tokens, 128), F32)),
            in_specs=[pl.BlockSpec(memory_space=pltpu.SMEM), hbm, hbm, hbm, hbm],
            out_specs=(vmem, vmem, vmem),
            scratch_shapes=[
                pltpu.VMEM((1, tokens), jnp.int32),
                pltpu.VMEM((tokens, hidden_size), BF16),
                pltpu.VMEM((hidden_size // 128, 128), BF16),
                pltpu.VMEM((hidden_size // 128, 128), F32),
                pltpu.VMEM((G * width, 128), BF16),
                pltpu.VMEM((NR, 2, G * R, width), BF16),
                pltpu.VMEM((NL, 2, G * R, width), BF16),
                pltpu.VMEM((4, G * rt, width), BF16),
            ] + [pltpu.VMEM((packed, 128), F32)] * 7 + [
                pltpu.VMEM((rt, 128), F32),
                pltpu.VMEM((3, 8, 128), F32),
                pltpu.VMEM((4, 8, 128), F32),
                pltpu.SemaphoreType.DMA((3,)),
                pltpu.SemaphoreType.DMA((NR, 2)),
                pltpu.SemaphoreType.DMA((NL, 2)),
            ] + [pltpu.SemaphoreType.DMA((n,)) for n in (2, NA, 2, NB, NS, NX, 8)],
            compiler_params=pltpu.CompilerParams(collective_id=0, has_side_effects=True,
                                                 vmem_limit_bytes=54 * 2 ** 20),
        )(temperature.reshape(1, 1), targets.reshape(1, tokens), hidden, final_gain.reshape(hidden_size // 128, 128), table)
        edges = [0, 1024, 3072, 7168] + list(range(13312, vq - 4096, 6144)) + [vq]
        log_norm, target_logprob, probs = pl.pallas_call(
            functools.partial(probs_kernel, edges),
            out_shape=(jax.ShapeDtypeStruct((1, tokens), F32),
                       jax.ShapeDtypeStruct((1, tokens), F32),
                       jax.ShapeDtypeStruct((tokens, vq), BF16)),
            in_specs=[vmem, vmem, vmem],
            out_specs=(hbm, hbm, hbm),
            scratch_shapes=[pltpu.VMEM((1, tokens), F32), pltpu.VMEM((1, tokens), F32),
                            pltpu.VMEM((tokens, vq), BF16),
                            pltpu.SemaphoreType.DMA((1,)), pltpu.SemaphoreType.DMA((2,))],
            compiler_params=pltpu.CompilerParams(vmem_limit_bytes=8 * 2 ** 20),
        )(exps, stats, scale)
        return log_norm.reshape(tokens), target_logprob.reshape(tokens), probs

    return jax.shard_map(local_scores, mesh=mesh,
                         in_specs=(P('dp', None), P(None), P(None, 'tp'), P('dp'), P()),
                         out_specs=(P('dp'), P('dp'), P('dp', 'tp')),
                         check_vma=False)
```
